32 devices in a mesh: dp: 16 (over z, y, x), mp: 2 (over core).
Axes of the slice: x: 2, y: 2, z: 4, core: 2. Of those that a mesh axis runs over, the one named last changes fastest.
Arguments:
- belief: bfloat16 [4096, 2652], P('dp'), may hold values from -6 to 6
- target_value: bfloat16 [4096, 1326], P('dp'), may hold values from -6 to 6
- counts: int32 [32], P('dp'), may hold values from 1 to 128, as said below
- w_first: bfloat16 [2652, 1536], P(None, 'mp'), may hold values from -0.125 to 0.125
- w_middle: bfloat16 [1536, 1536], P('mp'), may hold values from -0.15625 to 0.15625
- w_last: bfloat16 [1536, 1326], P(None, 'mp'), may hold values from -0.15625 to 0.15625
Outputs:
- grad_first: float32 [2652, 1536], P(None, ('mp', 'dp'))
- grad_middle: float32 [1536, 1536], P('mp', 'dp')
- grad_last: float32 [1536, 1326], P('dp', 'mp')
The draws below stay inside these ranges and needn't reach their ends.
Inputs may be any that keep to these rules, and one draw needn't show every extreme that they name: `counts`: rows past a subgame's count in its block are padding with arbitrary values.
All inputs are finite; a program needn't handle non-finite values.
Results may differ from the reference program's by a relative error of at most 0.0089.
Values may be sent and summed in bfloat16 or wider, within the bound.
A program may use at most 192 MiB of HBM per device.

```python
import jax
import jax.numpy as jnp
from jax import lax

IN = 2652
HID = 1536
OUT = 1326
BLOCK = 128
SUB_DEV = 2
ROWS = 4096
PARAMS = 8469504
N_DP = 16


def draw_counts(key, part):
    key_ceiling, key_counts, key_spot = jax.random.split(key, 3)
    ceiling = jax.random.randint(key_ceiling, (N_DP, 1), 48, BLOCK + 1)
    floor_level = ceiling // 2
    drawn = jax.random.randint(key_counts, (N_DP, SUB_DEV), floor_level, ceiling + 1)
    flat_counts = drawn.reshape(N_DP * SUB_DEV)
    spot = jax.random.randint(key_spot, (), 0, N_DP * SUB_DEV)
    return flat_counts.at[spot].set(BLOCK).astype(jnp.int32)


def steps_of(key, shape, shards, least, high):
    level = 1.0
    for position, parts in shards:
        steps = jax.random.uniform(jax.random.fold_in(jax.random.fold_in(key, 6), position), (parts,), jnp.float32, least / len(shards), high / len(shards))
        level = level * jnp.repeat(jnp.exp(steps), shape[position] // parts).reshape((-1,) + (1,) * (len(shape) - 1 - position))
    return level


def scatter_about(own_key, shape, scale, reach, cuts=(), kind=jnp.bfloat16):
    factor_of = steps_of(own_key, shape, cuts, -0.22, 0.18) if cuts else 1.0
    values = jax.random.normal(own_key, shape, jnp.float32) * scale * factor_of
    return jnp.minimum(jnp.maximum(values, -reach), reach).astype(kind)


def setup_inputs(seed: int = 0) -> dict:
    key_of = jax.random.split(jax.random.key(seed), 7)
    return {
        "belief": scatter_about(key_of[0], (ROWS, IN), 1.0, 6.0, ((0, 16),)),
        "target_value": scatter_about(key_of[1], (ROWS, OUT), 1.0, 6.0, ((0, 16),)),
        "counts": draw_counts(jax.random.fold_in(key_of[6], 71), 0),
        "w_first": scatter_about(key_of[3], (IN, HID), IN ** -0.5, 0.125, ((1, 2),)),
        "w_middle": scatter_about(key_of[4], (HID, HID), HID ** -0.5, 0.15625, ((0, 2),)),
        "w_last": scatter_about(key_of[5], (HID, OUT), HID ** -0.5, 0.15625, ((1, 2),)),
    }


def silu_slope(pre_act):
    sigmoid_of = jax.nn.sigmoid(pre_act)
    return sigmoid_of * (1.0 + pre_act * (1.0 - sigmoid_of))

def rows_grads(belief, target_value, live_mask, w_first, w_middle, w_last):
    pre_first = jnp.dot(belief, w_first, preferred_element_type=jnp.float32)
    act_first = jax.nn.silu(pre_first).astype(jnp.bfloat16)
    pre_middle = jnp.dot(act_first, w_middle, preferred_element_type=jnp.float32)
    act_middle = jax.nn.silu(pre_middle).astype(jnp.bfloat16)
    predicted = jnp.dot(act_middle, w_last, preferred_element_type=jnp.float32)
    mismatch = predicted - target_value.astype(jnp.float32)
    slope_out = (jnp.clip(mismatch, -1.0, 1.0) * live_mask[:, None]).astype(jnp.bfloat16)
    raw_last = jnp.dot(act_middle.T, slope_out, preferred_element_type=jnp.float32)
    back_middle = jnp.dot(slope_out, w_last.T, preferred_element_type=jnp.float32)
    slope_middle = (back_middle * silu_slope(pre_middle)).astype(jnp.bfloat16)
    raw_middle = jnp.dot(act_first.T, slope_middle, preferred_element_type=jnp.float32)
    back_first = jnp.dot(slope_middle, w_middle.T, preferred_element_type=jnp.float32)
    slope_first = (back_first * silu_slope(pre_first)).astype(jnp.bfloat16)
    raw_first = jnp.dot(belief.T, slope_first, preferred_element_type=jnp.float32)
    return (raw_first, raw_middle, raw_last)

def reference(belief, target_value, counts, w_first, w_middle, w_last):
    total_rows = belief.shape[0]
    span_rows = SUB_DEV * BLOCK
    block_count = total_rows // span_rows
    live_all = (counts[:, None] > jnp.arange(BLOCK, dtype=jnp.int32)[None, :]).astype(jnp.float32).reshape(total_rows)

    def add_block(running, block_index):
        row_start = (block_index * span_rows).astype(jnp.int32)
        part_belief = lax.dynamic_slice_in_dim(belief, row_start, span_rows, 0)
        part_target = lax.dynamic_slice_in_dim(target_value, row_start, span_rows, 0)
        part_live = lax.dynamic_slice_in_dim(live_all, row_start, span_rows, 0)
        pieces = rows_grads(part_belief, part_target, part_live, w_first, w_middle, w_last)
        return (tuple((left + right for left, right in zip(running, pieces))), None)
    zeros_init = (jnp.zeros(w_first.shape, jnp.float32), jnp.zeros(w_middle.shape, jnp.float32), jnp.zeros(w_last.shape, jnp.float32))
    running, _ = lax.scan(add_block, zeros_init, jnp.arange(block_count, dtype=jnp.int32))
    raw_first, raw_middle, raw_last = running
    square_sum = jnp.sum(raw_first * raw_first) + jnp.sum(raw_middle * raw_middle) + jnp.sum(raw_last * raw_last)
    norm_scale = lax.rsqrt(square_sum / PARAMS + 1e-06)
    return (raw_first * norm_scale, raw_middle * norm_scale, raw_last * norm_scale)
```

```python
import functools
import math

import jax
import jax.numpy as jnp
from jax import lax
from jax.experimental import pallas as pl
from jax.experimental.pallas import tpu as pltpu
from jax.sharding import PartitionSpec as P

BLOCK = 128
LANES = 128
MESH = pl.DeviceIdType.MESH
FIRST, MIDDLE, LAST = 0, 1, 2
NT = (((1,), (1,)), ((), ()))


def silu_slope(pre_act):
    sigmoid_of = jax.nn.sigmoid(pre_act)
    return sigmoid_of * (1.0 + pre_act * (1.0 - sigmoid_of))


def pad_to(size, step):
    return -(-size // step) * step


def orders_of(n_dp):
    bits = n_dp.bit_length() - 1
    heads = {FIRST: (0, 1), MIDDLE: (2, 0, 1), LAST: (1, 0)}
    return {
        which: head + tuple(b for b in range(bits) if b not in head)
        for which, head in heads.items()
    }


def pieces_of(wide):
    out = []
    for which, keys in (
        (MIDDLE, (27, 33)),
        (FIRST, (28, 34, 41, 47)),
        (LAST, (39, 45)),
    ):
        tiles = wide[which] // LANES
        parts = len(keys)
        bounds = [round(tiles * i / parts) * LANES for i in range(parts + 1)]
        for i, key in enumerate(keys):
            out.append((which, bounds[i], bounds[i + 1] - bounds[i], key))
    return out


def step_kernel(dims, params, orders, pieces, stage_shapes, *refs):
    n_dp, n_mp = dims
    stages = n_dp.bit_length() - 2
    count = len(pieces)
    counts, loads, outs, scale_out = refs[0], refs[1:6], refs[6:9], refs[9]
    refs = refs[10:]
    held = [refs[k * count : (k + 1) * count] for k in range(stages)]
    refs = refs[stages * count :]
    got = [refs[k * count : (k + 1) * count] for k in range(stages)]
    refs = refs[stages * count :]
    belief_t, target_t, w_first, w_middle, w_last_t = refs[:5]
    parts_t, near_t = refs[5:8], refs[8:11]
    (
        belief, near_belief, pre1, act1, near_act1, part2, other2, pre2, act2, slope_out, near_out,
        part_back, other_back, slope2, slope1, load_sems, swap_send, swap_got, share_send, share_got,
        sends, gots, sq_send, sq_got, sq_sems,
    ) = refs[11:]

    in_width, own_hid = w_first.shape
    own_width, hid = w_last_t.shape
    rows = belief.shape[0]
    blocks = part2.shape[0]
    block = hid // blocks

    landing = (belief_t, target_t, w_first, w_middle, w_last_t)
    arrivals = [
        pltpu.make_async_copy(src, dst, load_sems.at[i])
        for i, (src, dst) in enumerate(zip(loads, landing))
    ]
    for i in (0, 2, 3, 4, 1):
        arrivals[i].start()

    dp, mp = lax.axis_index("dp"), lax.axis_index("mp")
    me = dp * n_mp + mp
    total = n_dp * n_mp

    def side(bit):
        return (dp // (1 << bit)) % 2

    def peer(bit):
        return (dp + (1 - 2 * side(bit)) * (1 << bit), mp)

    sibling = (dp, 1 - mp)
    barrier = pltpu.get_barrier_semaphore()

    def greet(j, _):
        other = lax.rem(me + j, total)
        pl.semaphore_signal(
            barrier, inc=1, device_id=(other // n_mp, other % n_mp), device_id_type=MESH
        )
        return 0

    lax.fori_loop(1, total, greet, 0)

    def remote(src, dst, sems, k, goal):
        return pltpu.make_async_remote_copy(
            src, dst, sems[0].at[k], sems[1].at[k], device_id=goal, device_id_type=MESH
        )

    share = functools.partial(remote, sems=(share_send, share_got))
    my_rows = pl.ds(pl.multiple_of(mp * (rows // 2), rows // 2), rows // 2)
    pair = {which: orders[which][0] for which in orders}
    away = {which: 1 - side(pair[which]) for which in orders}
    home = {which: side(pair[which]) for which in orders}
    send_belief = share(
        belief.at[my_rows, :], near_belief.at[my_rows, :], k=0, goal=peer(pair[FIRST])
    )
    send_act1 = share(act1, near_act1, k=1, goal=peer(pair[MIDDLE]))
    send_act2 = share(
        parts_t[LAST].at[away[LAST], mp], near_t[LAST].at[mp], k=2, goal=peer(pair[LAST])
    )
    send_out = share(slope_out, near_out, k=3, goal=peer(pair[LAST]))
    send_slope2 = share(
        parts_t[MIDDLE].at[away[MIDDLE], mp], near_t[MIDDLE].at[mp], k=4, goal=peer(pair[MIDDLE])
    )
    send_slope1 = share(parts_t[FIRST].at[away[FIRST]], near_t[FIRST], k=5, goal=peer(pair[FIRST]))
    pass_belief = share(
        near_belief.at[my_rows, :], near_belief.at[my_rows, :], k=6, goal=sibling
    )
    pass_act2 = share(near_t[LAST].at[mp], near_t[LAST].at[mp], k=7, goal=sibling)
    pass_slope2 = share(near_t[MIDDLE].at[mp], near_t[MIDDLE].at[mp], k=8, goal=sibling)

    def swap(way, part, other, i):
        return pltpu.make_async_remote_copy(
            part.at[i], other.at[i], swap_send.at[way, i], swap_got.at[way, i],
            device_id=sibling, device_id_type=MESH,
        )

    def transpose_parts(which, source, width):
        order = orders[which]
        r = width // n_dp
        step = math.lcm(r, LANES)
        for start in range(0, width, step):
            value = source[:, start : start + step].T
            for d in range(start // r, (start + step) // r):
                where = [(d >> bit) & 1 for bit in order]
                at = 0
                for bit in where[2:]:
                    at = 2 * at + bit
                parts_t[which][where[0], where[1], at * r : (at + 1) * r, :] = value[
                    d * r - start : (d + 1) * r - start
                ]

    rights = {FIRST: (belief, near_belief), MIDDLE: (act1, near_act1), LAST: (slope_out, near_out)}

    def weight_grad(p, half):
        which, start, width, _ = pieces[p]
        own, near = rights[which]
        value = jnp.dot(
            parts_t[which][home[which], half], own[:, start : start + width],
            preferred_element_type=jnp.float32,
        ) + jnp.dot(
            near_t[which][half], near[:, start : start + width],
            preferred_element_type=jnp.float32,
        )
        store(p, 0, half, value)

    def store(p, k, half, value):
        ref = held[k][p]
        if k == stages - 1:
            ref[half] = value.astype(jnp.bfloat16)
            return
        h = value.shape[0] // 2
        ref[half, 0] = value[:h].astype(jnp.bfloat16)
        ref[half, 1] = value[h:].astype(jnp.bfloat16)

    def exchange(p, k):
        bit = orders[pieces[p][0]][1 + k]
        return pltpu.make_async_remote_copy(
            held[k][p].at[1 - side(bit)], got[k][p], sends.at[k, p], gots.at[k, p],
            device_id=peer(bit), device_id_type=MESH,
        )

    def send_grad(p):
        weight_grad(p, 1 - side(orders[pieces[p][0]][1]))
        exchange(p, 0).start()

    def keep_grad(p):
        weight_grad(p, side(orders[pieces[p][0]][1]))

    arrivals[0].wait()
    for start in range(0, belief.shape[1], LANES * 3):
        value = belief_t[start : min(start + LANES * 3, in_width), :]
        if value.shape[0] < LANES * 3:
            value = jnp.concatenate(
                [value, jnp.zeros((LANES * 3 - value.shape[0], rows), jnp.bfloat16)], axis=0
            )
        belief[:, start : start + LANES * 3] = value.T
    pl.semaphore_wait(barrier, total - 1)
    send_belief.start()
    arrivals[2].wait()
    for c in range(0, own_hid, 256):
        value = jnp.dot(
            belief[:, :in_width], w_first[:, c : c + 256], preferred_element_type=jnp.float32
        )
        pre1[:, c : c + 256] = value
        act1[:, c : c + 256] = jax.nn.silu(value).astype(jnp.bfloat16)
    send_act1.start()
    arrivals[3].wait()
    for i in range(blocks):
        part2[i] = jnp.dot(
            act1[...], w_middle[:, i * block : (i + 1) * block],
            preferred_element_type=jnp.float32,
        )
        swap(0, part2, other2, i).start()
    arrivals[1].wait()
    arrivals[4].wait()
    row = lax.broadcasted_iota(jnp.int32, (rows, 1), 0)
    limit = jnp.full((rows, 1), counts[0], jnp.int32)
    for b in range(1, rows // BLOCK):
        limit = jnp.where(row >= b * BLOCK, counts[b] + b * BLOCK, limit)
    live = jnp.where(row < limit, 1.0, 0.0)
    target = target_t[...].T
    wanted = target[:, :own_width].astype(jnp.float32)
    for m in range(1, n_mp):
        wanted = jnp.where(
            mp == m, target[:, m * own_width : (m + 1) * own_width].astype(jnp.float32), wanted
        )
    for i in range(blocks):
        cols = slice(i * block, (i + 1) * block)
        swap(0, part2, other2, i).wait_recv()
        value = part2[i] + other2[i]
        pre2[:, cols] = value
        act2[:, cols] = jax.nn.silu(value).astype(jnp.bfloat16)
    transpose_parts(LAST, act2, hid)
    send_act2.start()
    predicted = lax.dot_general(act2[...], w_last_t[...], NT, preferred_element_type=jnp.float32)
    value = jnp.clip(predicted - wanted, -1.0, 1.0) * live
    slope_out[...] = jnp.concatenate(
        [value, jnp.zeros((rows, slope_out.shape[1] - own_width), jnp.float32)], axis=1
    ).astype(jnp.bfloat16)
    send_out.start()

    for i in range(blocks):
        part_back[i] = jnp.dot(
            slope_out[:, :own_width], w_last_t[:, i * block : (i + 1) * block],
            preferred_element_type=jnp.float32,
        )
        swap(1, part_back, other_back, i).start()
    for i in range(blocks):
        cols = slice(i * block, (i + 1) * block)
        swap(1, part_back, other_back, i).wait_recv()
        value = (part_back[i] + other_back[i]) * silu_slope(pre2[:, cols])
        slope2[:, cols] = value.astype(jnp.bfloat16)
    transpose_parts(MIDDLE, slope2, hid)
    send_slope2.start()
    for c in range(0, own_hid, 256):
        back = lax.dot_general(
            slope2[...], w_middle[c : c + 256, :], NT, preferred_element_type=jnp.float32
        )
        slope1[:, c : c + 256] = (back * silu_slope(pre1[:, c : c + 256])).astype(jnp.bfloat16)
    transpose_parts(FIRST, slope1, own_hid)
    send_slope1.start()

    send_act2.wait_recv()
    pass_act2.start()
    send_belief.wait_recv()
    pass_belief.start()
    send_slope2.wait_recv()
    pass_slope2.start()
    send_act1.wait_recv()
    pass_slope2.wait_recv()
    by_layer = {which: [p for p in range(count) if pieces[p][0] == which] for which in orders}
    late = by_layer[FIRST][2:]
    for p in by_layer[MIDDLE]:
        send_grad(p)
    pass_belief.wait_recv()
    send_slope1.wait_recv()
    for p in by_layer[FIRST][:2]:
        send_grad(p)
    pass_act2.wait_recv()
    send_out.wait_recv()
    for p in by_layer[LAST]:
        send_grad(p)
    for p in range(count):
        if p not in late:
            keep_grad(p)

    steps = sorted(
        (pieces[p][3] + 7 * k, k, p) for p in range(count) for k in range(stages - 1)
    )
    for _, k, p in steps:
        if late:
            send_grad(late[0])
            keep_grad(late[0])
            late = late[1:]
        bit = orders[pieces[p][0]][1 + k]
        exchange(p, k).wait_recv()
        for h in range(2):
            value = held[k][p][side(bit), h].astype(jnp.float32) + got[k][p][h].astype(jnp.float32)
            store(p, k + 1, h, value)
        exchange(p, k + 1).start()

    squares = jnp.float32(0.0)
    for p in sorted(range(count), key=lambda p: pieces[p][3]):
        which, start, width, _ = pieces[p]
        k = stages - 1
        bit = orders[which][1 + k]
        exchange(p, k).wait_recv()
        value = held[k][p][side(bit)].astype(jnp.float32) + got[k][p][...].astype(jnp.float32)
        outs[which][:, start : start + width] = value
        squares = squares + jnp.sum(value * value)

    sq_send[...] = jnp.full(sq_send.shape, squares, jnp.float32)

    def square_copy(j):
        other = lax.rem(me + j, total)
        return pltpu.make_async_remote_copy(
            sq_send, sq_got.at[j - 1], sq_sems.at[0], sq_sems.at[1],
            device_id=(other // n_mp, other % n_mp), device_id_type=MESH,
        )

    def tell(j, _):
        square_copy(j).start()
        return 0

    lax.fori_loop(1, total, tell, 0)
    for i in range(blocks):
        swap(0, part2, other2, i).wait_send()
        swap(1, part_back, other_back, i).wait_send()
    for copy in (
        send_belief, send_act1, send_act2, send_out, send_slope2, send_slope1,
        pass_belief, pass_act2, pass_slope2,
    ):
        copy.wait_send()
    for p in range(count):
        for k in range(stages):
            exchange(p, k).wait_send()
    pltpu.make_async_copy(sq_got, sq_got, sq_sems.at[1]).wait()
    everyone = squares + jnp.sum(sq_got[...]) * (1.0 / (sq_send.shape[0] * sq_send.shape[1]))
    scale_out[...] = lax.rsqrt(
        jnp.full(scale_out.shape, everyone / params + 1e-06, jnp.float32)
    )
    pltpu.make_async_copy(sq_got, sq_got, sq_sems.at[0]).wait()


def scale_kernel(scale, *refs):
    factor = scale[0:1, 0:1]
    for raw, out in zip(refs[:3], refs[3:]):
        out[...] = raw[:, : out.shape[1]] * factor


def per_device(dims, belief, target_value, counts, w_first, w_middle, w_last):
    n_dp, n_mp = dims
    stages = n_dp.bit_length() - 2
    blocks = 3
    rows, (in_width, own_hid) = belief.shape[0], w_first.shape
    hid, own_width = w_last.shape
    params = float(n_mp * (w_first.size + w_middle.size + w_last.size))
    long = {FIRST: own_hid, MIDDLE: hid, LAST: hid}
    wide = {
        FIRST: pad_to(in_width, LANES),
        MIDDLE: pad_to(own_hid, LANES),
        LAST: pad_to(own_width, LANES),
    }
    layers = (FIRST, MIDDLE, LAST)
    orders = orders_of(n_dp)
    pieces = pieces_of(wide)
    half, single = jnp.bfloat16, jnp.float32

    def stage_shape(piece, k):
        r = long[piece[0]] // 2 >> (k + 1)
        return (2, r, piece[2]) if k == stages - 1 else (2, 2, r // 2, piece[2])

    shapes = [[stage_shape(piece, k) for piece in pieces] for k in range(stages)]
    loads = (belief.T, target_value.T, w_first, w_middle, w_last.T)
    swapped = pltpu.VMEM((blocks, rows, hid // blocks), single)
    count = len(pieces)
    raws = pl.pallas_call(
        functools.partial(step_kernel, dims, params, orders, pieces, shapes),
        out_shape=[
            jax.ShapeDtypeStruct((long[w] // n_dp, wide[w]), single) for w in layers
        ] + [jax.ShapeDtypeStruct((8, LANES), single)],
        in_specs=[pl.BlockSpec(memory_space=pltpu.SMEM)]
        + [pl.BlockSpec(memory_space=pl.ANY)] * 5,
        out_specs=[pl.BlockSpec(memory_space=pltpu.VMEM)] * 4,
        scratch_shapes=(
            [pltpu.VMEM(s, half) for stage in shapes for s in stage]
            + [pltpu.VMEM(s[1:], half) for stage in shapes for s in stage]
            + [
                pltpu.VMEM((in_width, rows), half),
                pltpu.VMEM((n_mp * own_width, rows), half),
                pltpu.VMEM(w_first.shape, half),
                pltpu.VMEM(w_middle.shape, half),
                pltpu.VMEM((own_width, hid), half),
            ]
            + [pltpu.VMEM((2, 2, long[w] // 4, rows), half) for w in layers]
            + [pltpu.VMEM((2, long[w] // 4, rows), half) for w in layers]
            + [
                pltpu.VMEM((rows, wide[FIRST]), half),
                pltpu.VMEM((rows, wide[FIRST]), half),
                pltpu.VMEM((rows, own_hid), single),
                pltpu.VMEM((rows, own_hid), half),
                pltpu.VMEM((rows, own_hid), half),
                swapped,
                swapped,
                pltpu.VMEM((rows, hid), single),
                pltpu.VMEM((rows, hid), half),
                pltpu.VMEM((rows, wide[LAST]), half),
                pltpu.VMEM((rows, wide[LAST]), half),
                swapped,
                swapped,
                pltpu.VMEM((rows, hid), half),
                pltpu.VMEM((rows, own_hid), half),
                pltpu.SemaphoreType.DMA((5,)),
                pltpu.SemaphoreType.DMA((2, blocks)),
                pltpu.SemaphoreType.DMA((2, blocks)),
                pltpu.SemaphoreType.DMA((9,)),
                pltpu.SemaphoreType.DMA((9,)),
                pltpu.SemaphoreType.DMA((stages, count)),
                pltpu.SemaphoreType.DMA((stages, count)),
                pltpu.VMEM((8, LANES), single),
                pltpu.VMEM((n_dp * n_mp - 1, 8, LANES), single),
                pltpu.SemaphoreType.DMA((2,)),
            ]
        ),
        compiler_params=pltpu.CompilerParams(
            collective_id=0, has_side_effects=True, vmem_limit_bytes=60 * 1024 * 1024
        ),
    )(counts, *loads)
    finals = (
        (long[FIRST] // n_dp, in_width),
        (long[MIDDLE] // n_dp, own_hid),
        (long[LAST] // n_dp, own_width),
    )
    first, middle, last = pl.pallas_call(
        scale_kernel,
        out_shape=[jax.ShapeDtypeStruct(s, single) for s in finals],
        in_specs=[pl.BlockSpec(memory_space=pltpu.VMEM)] * 4,
        out_specs=[pl.BlockSpec(memory_space=pltpu.VMEM)] * 3,
    )(raws[3], *raws[:3])
    return first.T, middle.T, last


def solution(mesh):
    return jax.shard_map(
        functools.partial(per_device, (mesh.shape["dp"], mesh.shape["mp"])),
        mesh=mesh,
        in_specs=(
            P("dp", None),
            P("dp", None),
            P("dp"),
            P(None, "mp"),
            P("mp", None),
            P(None, "mp"),
        ),
        out_specs=(P(None, ("mp", "dp")), P("mp", "dp"), P("dp", "mp")),
        check_vma=False,
    )
```

```python
import functools
import math

import jax
import jax.numpy as jnp
from jax import lax
from jax.experimental import pallas as pl
from jax.experimental.pallas import tpu as pltpu
from jax.sharding import PartitionSpec as P

BLOCK = 128
LANES = 128
MESH = pl.DeviceIdType.MESH
FIRST, MIDDLE, LAST = 0, 1, 2
NT = (((1,), (1,)), ((), ()))


def silu_slope(pre_act):
    sigmoid_of = jax.nn.sigmoid(pre_act)
    return sigmoid_of * (1.0 + pre_act * (1.0 - sigmoid_of))


def pad_to(size, step):
    return -(-size // step) * step


def orders_of(n_dp):
    bits = n_dp.bit_length() - 1
    heads = {FIRST: ((0, 1), (2,)), MIDDLE: ((2,), (1, 0)), LAST: ((2,), (0, 1))}
    return {
        which: (shared, head + tuple(b for b in range(bits) if b not in shared + head))
        for which, (shared, head) in heads.items()
    }


def pieces_of(wide):
    out = []
    for which, table in (
        (LAST, ((36.7, 44.6, 50), (43, 51, 55))),
        (FIRST, ((36, 41), (38.7, 44), (41.8, 47), (44.5, 49))),
        (MIDDLE, ((41.5, 46.8, 52), (47.8, 53, 57))),
    ):
        tiles = wide[which] // LANES
        parts = len(table)
        bounds = [round(tiles * i / parts) * LANES for i in range(parts + 1)]
        for i, keys in enumerate(table):
            out.append((which, bounds[i], bounds[i + 1] - bounds[i], keys))
    return out


def step_kernel(dims, params, orders, pieces, stage_shapes, *refs):
    n_dp, n_mp = dims
    count = len(pieces)
    counts, loads, outs, scale_out = refs[0], refs[1:6], refs[6:9], refs[9]
    refs = refs[10:]
    held, got = [], []
    for group in (held, got):
        for shapes in stage_shapes:
            group.append(refs[: len(shapes)])
            refs = refs[len(shapes) :]
    belief_t, target_t, w_first, w_middle, w_last_t = refs[:5]
    parts_t, near_t = refs[5:8], refs[8:11]
    (
        belief, near_belief, pre1, act1, near_act1, part2, other2, pre2, act2, slope_out, near_out,
        part_back, other_back, slope2, slope1, load_sems, swap_send, swap_got, share_send, share_got,
        sends, gots, sq_send, sq_got, sq_sems,
    ) = refs[11:]

    in_width, own_hid = w_first.shape
    own_width, hid = w_last_t.shape
    rows = belief.shape[0]
    blocks = part2.shape[0]
    block = hid // blocks

    landing = (belief_t, target_t, w_first, w_middle, w_last_t)
    arrivals = [
        pltpu.make_async_copy(src, dst, load_sems.at[i])
        for i, (src, dst) in enumerate(zip(loads, landing))
    ]
    for i in (0, 2, 3, 4, 1):
        arrivals[i].start()

    dp, mp = lax.axis_index("dp"), lax.axis_index("mp")
    me = dp * n_mp + mp
    total = n_dp * n_mp

    def side(bit):
        return (dp // (1 << bit)) % 2

    def peer(bit):
        return (dp + (1 - 2 * side(bit)) * (1 << bit), mp)

    sibling = (dp, 1 - mp)
    barrier = pltpu.get_barrier_semaphore()

    def greet(j, _):
        other = lax.rem(me + j, total)
        pl.semaphore_signal(
            barrier, inc=1, device_id=(other // n_mp, other % n_mp), device_id_type=MESH
        )
        return 0

    lax.fori_loop(1, total, greet, 0)

    def remote(src, dst, sems, k, goal):
        return pltpu.make_async_remote_copy(
            src, dst, sems[0].at[k], sems[1].at[k], device_id=goal, device_id_type=MESH
        )

    share = functools.partial(remote, sems=(share_send, share_got))
    my_rows = pl.ds(pl.multiple_of(mp * (rows // 2), rows // 2), rows // 2)
    x, y = (side(bit) for bit in orders[FIRST][0])
    x_peer, y_peer = (peer(bit) for bit in orders[FIRST][0])
    diagonal = (x_peer[0] + y_peer[0] - dp, mp)
    (low,) = orders[MIDDLE][0]
    z, z_peer = side(low), peer(low)
    belief_x = share(belief.at[my_rows, :], near_belief.at[0, my_rows, :], k=0, goal=x_peer)
    belief_y = share(belief.at[my_rows, :], near_belief.at[1, my_rows, :], k=1, goal=y_peer)
    relay_goal = (jnp.where(mp == 0, y_peer[0], x_peer[0]), mp)
    relay = share(
        near_belief.at[mp, my_rows, :], near_belief.at[2, my_rows, :], k=2, goal=relay_goal
    )
    passes = [
        share(near_belief.at[i, my_rows, :], near_belief.at[i, my_rows, :], k=3 + i, goal=sibling)
        for i in range(3)
    ]
    slopes = [
        share(parts_t[FIRST].at[at], near_t[FIRST].at[i], k=6 + i, goal=goal)
        for i, (at, goal) in enumerate(
            (((1 - x, y), x_peer), ((x, 1 - y), y_peer), ((1 - x, 1 - y), diagonal))
        )
    ]
    send_act1 = share(act1, near_act1, k=9, goal=z_peer)
    send_act2 = share(parts_t[LAST].at[1 - z, mp], near_t[LAST].at[mp], k=10, goal=z_peer)
    send_out = share(slope_out, near_out, k=11, goal=z_peer)
    send_slope2 = share(parts_t[MIDDLE].at[1 - z, mp], near_t[MIDDLE].at[mp], k=12, goal=z_peer)
    pass_act2 = share(near_t[LAST].at[mp], near_t[LAST].at[mp], k=13, goal=sibling)
    pass_slope2 = share(near_t[MIDDLE].at[mp], near_t[MIDDLE].at[mp], k=14, goal=sibling)

    def swap(way, part, other, i):
        return pltpu.make_async_remote_copy(
            part.at[i], other.at[i], swap_send.at[way, i], swap_got.at[way, i],
            device_id=sibling, device_id_type=MESH,
        )

    def transpose_parts(which, source, width):
        order = orders[which][0] + orders[which][1]
        r = width // n_dp
        step = math.lcm(r, LANES)
        for start in range(0, width, step):
            value = source[:, start : start + step].T
            for d in range(start // r, (start + step) // r):
                where = [(d >> bit) & 1 for bit in order]
                at = 0
                for bit in where[2:]:
                    at = 2 * at + bit
                parts_t[which][where[0], where[1], at * r : (at + 1) * r, :] = value[
                    d * r - start : (d + 1) * r - start
                ]

    def dot(left, right):
        return jnp.dot(left, right, preferred_element_type=jnp.float32)

    def first_grad(p):
        _, start, width, _ = pieces[p]
        cols = slice(start, start + width)
        value = dot(parts_t[FIRST][x, y], belief[:, cols])
        for i in range(3):
            value = value + dot(near_t[FIRST][i], near_belief[i, :, cols])
        h = value.shape[0] // 2
        store(p, 0, 0, value[:h])
        store(p, 0, 1, value[h:])
        exchange(p, 0).start()

    rights = {MIDDLE: (act1, near_act1), LAST: (slope_out, near_out)}

    def pair_grad(p, half):
        which, start, width, _ = pieces[p]
        own, near = rights[which]
        cols = slice(start, start + width)
        value = dot(parts_t[which][z, half], own[:, cols]) + dot(near_t[which][half], near[:, cols])
        store(p, 0, half, value)

    def stages_of(p):
        return len(orders[pieces[p][0]][1])

    def store(p, k, half, value):
        ref = held[p][k]
        if k == stages_of(p) - 1:
            ref[half] = value.astype(jnp.bfloat16)
            return
        h = value.shape[0] // 2
        ref[half, 0] = value[:h].astype(jnp.bfloat16)
        ref[half, 1] = value[h:].astype(jnp.bfloat16)

    def exchange(p, k):
        bit = orders[pieces[p][0]][1][k]
        return pltpu.make_async_remote_copy(
            held[p][k].at[1 - side(bit)], got[p][k], sends.at[p, k], gots.at[p, k],
            device_id=peer(bit), device_id_type=MESH,
        )

    def send_grad(p):
        pair_grad(p, 1 - side(orders[pieces[p][0]][1][0]))
        exchange(p, 0).start()

    def keep_grad(p):
        pair_grad(p, side(orders[pieces[p][0]][1][0]))

    arrivals[0].wait()
    for start in range(0, belief.shape[1], LANES * 3):
        value = belief_t[start : min(start + LANES * 3, in_width), :]
        if value.shape[0] < LANES * 3:
            value = jnp.concatenate(
                [value, jnp.zeros((LANES * 3 - value.shape[0], rows), jnp.bfloat16)], axis=0
            )
        belief[:, start : start + LANES * 3] = value.T
    pl.semaphore_wait(barrier, total - 1)
    belief_x.start()
    belief_y.start()
    arrivals[2].wait()
    for c in range(0, own_hid, 256):
        value = jnp.dot(
            belief[:, :in_width], w_first[:, c : c + 256], preferred_element_type=jnp.float32
        )
        pre1[:, c : c + 256] = value
        act1[:, c : c + 256] = jax.nn.silu(value).astype(jnp.bfloat16)
    send_act1.start()
    arrivals[3].wait()
    for i in range(blocks):
        part2[i] = jnp.dot(
            act1[...], w_middle[:, i * block : (i + 1) * block],
            preferred_element_type=jnp.float32,
        )
        swap(0, part2, other2, i).start()
    arrivals[1].wait()
    arrivals[4].wait()
    row = lax.broadcasted_iota(jnp.int32, (rows, 1), 0)
    limit = jnp.full((rows, 1), counts[0], jnp.int32)
    for b in range(1, rows // BLOCK):
        limit = jnp.where(row >= b * BLOCK, counts[b] + b * BLOCK, limit)
    live = jnp.where(row < limit, 1.0, 0.0)
    target = target_t[...].T
    wanted = target[:, :own_width].astype(jnp.float32)
    for m in range(1, n_mp):
        wanted = jnp.where(
            mp == m, target[:, m * own_width : (m + 1) * own_width].astype(jnp.float32), wanted
        )
    for i in range(blocks):
        cols = slice(i * block, (i + 1) * block)
        swap(0, part2, other2, i).wait_recv()
        value = part2[i] + other2[i]
        pre2[:, cols] = value
        act2[:, cols] = jax.nn.silu(value).astype(jnp.bfloat16)
    transpose_parts(LAST, act2, hid)
    send_act2.start()
    predicted = lax.dot_general(act2[...], w_last_t[...], NT, preferred_element_type=jnp.float32)
    value = jnp.clip(predicted - wanted, -1.0, 1.0) * live
    slope_out[...] = jnp.concatenate(
        [value, jnp.zeros((rows, slope_out.shape[1] - own_width), jnp.float32)], axis=1
    ).astype(jnp.bfloat16)
    send_out.start()

    for i in range(blocks):
        part_back[i] = jnp.dot(
            slope_out[:, :own_width], w_last_t[:, i * block : (i + 1) * block],
            preferred_element_type=jnp.float32,
        )
        swap(1, part_back, other_back, i).start()
    for i in range(blocks):
        cols = slice(i * block, (i + 1) * block)
        swap(1, part_back, other_back, i).wait_recv()
        value = (part_back[i] + other_back[i]) * silu_slope(pre2[:, cols])
        slope2[:, cols] = value.astype(jnp.bfloat16)
    transpose_parts(MIDDLE, slope2, hid)
    send_slope2.start()
    for c in range(0, own_hid, 256):
        back = lax.dot_general(
            slope2[...], w_middle[c : c + 256, :], NT, preferred_element_type=jnp.float32
        )
        slope1[:, c : c + 256] = (back * silu_slope(pre1[:, c : c + 256])).astype(jnp.bfloat16)
    transpose_parts(FIRST, slope1, own_hid)
    for copy in slopes:
        copy.start()

    by_layer = {which: [p for p in range(count) if pieces[p][0] == which] for which in orders}
    send_act2.wait_recv()
    pass_act2.start()
    belief_x.wait_recv()
    belief_y.wait_recv()
    relay.start()
    passes[0].start()
    passes[1].start()
    pass_act2.wait_recv()
    send_out.wait_recv()
    for p in by_layer[LAST]:
        send_grad(p)
    for p in by_layer[LAST]:
        keep_grad(p)
    relay.wait_recv()
    passes[2].start()
    send_slope2.wait_recv()
    pass_slope2.start()
    slopes[0].wait_recv()
    slopes[1].wait_recv()
    slopes[2].wait_recv()
    passes[0].wait_recv()
    passes[1].wait_recv()
    passes[2].wait_recv()
    for p in by_layer[FIRST][:2]:
        first_grad(p)
    send_act1.wait_recv()
    pass_slope2.wait_recv()
    for p in by_layer[MIDDLE]:
        send_grad(p)
    for p in by_layer[FIRST][2:]:
        first_grad(p)
    for p in by_layer[MIDDLE]:
        keep_grad(p)

    steps = []
    for p in range(count):
        keys = pieces[p][3]
        for k in range(stages_of(p)):
            steps.append((keys[min(k, len(keys) - 1)] + 7 * max(0, k + 1 - len(keys)), k, p))
    squares = jnp.float32(0.0)
    for _, k, p in sorted(steps):
        which, start, width, _ = pieces[p]
        mine = side(orders[which][1][k])
        exchange(p, k).wait_recv()
        if k < stages_of(p) - 1:
            for h in range(2):
                value = held[p][k][mine, h].astype(jnp.float32) + got[p][k][h].astype(jnp.float32)
                store(p, k + 1, h, value)
            exchange(p, k + 1).start()
        else:
            value = held[p][k][mine].astype(jnp.float32) + got[p][k][...].astype(jnp.float32)
            outs[which][:, start : start + width] = value
            squares = squares + jnp.sum(value * value)

    sq_send[...] = jnp.full(sq_send.shape, squares, jnp.float32)

    def square_copy(j):
        other = lax.rem(me + j, total)
        return pltpu.make_async_remote_copy(
            sq_send, sq_got.at[j - 1], sq_sems.at[0], sq_sems.at[1],
            device_id=(other // n_mp, other % n_mp), device_id_type=MESH,
        )

    def tell(j, _):
        square_copy(j).start()
        return 0

    lax.fori_loop(1, total, tell, 0)
    for i in range(blocks):
        swap(0, part2, other2, i).wait_send()
        swap(1, part_back, other_back, i).wait_send()
    for copy in (
        belief_x, belief_y, relay, *passes, *slopes,
        send_act1, send_act2, send_out, send_slope2, pass_act2, pass_slope2,
    ):
        copy.wait_send()
    for p in range(count):
        for k in range(stages_of(p)):
            exchange(p, k).wait_send()
    pltpu.make_async_copy(sq_got, sq_got, sq_sems.at[1]).wait()
    everyone = squares + jnp.sum(sq_got[...]) * (1.0 / (sq_send.shape[0] * sq_send.shape[1]))
    scale_out[...] = lax.rsqrt(
        jnp.full(scale_out.shape, everyone / params + 1e-06, jnp.float32)
    )
    pltpu.make_async_copy(sq_got, sq_got, sq_sems.at[0]).wait()


def scale_kernel(scale, *refs):
    factor = scale[0:1, 0:1]
    for raw, out in zip(refs[:3], refs[3:]):
        out[...] = raw[:, : out.shape[1]] * factor


def per_device(dims, belief, target_value, counts, w_first, w_middle, w_last):
    n_dp, n_mp = dims
    blocks = 3
    rows, (in_width, own_hid) = belief.shape[0], w_first.shape
    hid, own_width = w_last.shape
    params = float(n_mp * (w_first.size + w_middle.size + w_last.size))
    long = {FIRST: own_hid, MIDDLE: hid, LAST: hid}
    wide = {
        FIRST: pad_to(in_width, LANES),
        MIDDLE: pad_to(own_hid, LANES),
        LAST: pad_to(own_width, LANES),
    }
    layers = (FIRST, MIDDLE, LAST)
    orders = orders_of(n_dp)
    pieces = pieces_of(wide)
    half, single = jnp.bfloat16, jnp.float32

    def stage_shapes(piece):
        shared, rest = orders[piece[0]]
        for k in range(len(rest)):
            r = long[piece[0]] >> (len(shared) + k + 1)
            yield (2, r, piece[2]) if k == len(rest) - 1 else (2, 2, r // 2, piece[2])

    shapes = [list(stage_shapes(piece)) for piece in pieces]
    deepest = max(len(stages) for stages in shapes)
    loads = (belief.T, target_value.T, w_first, w_middle, w_last.T)
    swapped = pltpu.VMEM((blocks, rows, hid // blocks), single)
    count = len(pieces)
    raws = pl.pallas_call(
        functools.partial(step_kernel, dims, params, orders, pieces, shapes),
        out_shape=[
            jax.ShapeDtypeStruct((long[w] // n_dp, wide[w]), single) for w in layers
        ] + [jax.ShapeDtypeStruct((8, LANES), single)],
        in_specs=[pl.BlockSpec(memory_space=pltpu.SMEM)]
        + [pl.BlockSpec(memory_space=pl.ANY)] * 5,
        out_specs=[pl.BlockSpec(memory_space=pltpu.VMEM)] * 4,
        scratch_shapes=(
            [pltpu.VMEM(s, half) for stages in shapes for s in stages]
            + [pltpu.VMEM(s[1:], half) for stages in shapes for s in stages]
            + [
                pltpu.VMEM((in_width, rows), half),
                pltpu.VMEM((n_mp * own_width, rows), half),
                pltpu.VMEM(w_first.shape, half),
                pltpu.VMEM(w_middle.shape, half),
                pltpu.VMEM((own_width, hid), half),
            ]
            + [pltpu.VMEM((2, 2, long[w] // 4, rows), half) for w in layers]
            + [pltpu.VMEM((3 if w == FIRST else 2, long[w] // 4, rows), half) for w in layers]
            + [
                pltpu.VMEM((rows, wide[FIRST]), half),
                pltpu.VMEM((3, rows, wide[FIRST]), half),
                pltpu.VMEM((rows, own_hid), single),
                pltpu.VMEM((rows, own_hid), half),
                pltpu.VMEM((rows, own_hid), half),
                swapped,
                swapped,
                pltpu.VMEM((rows, hid), single),
                pltpu.VMEM((rows, hid), half),
                pltpu.VMEM((rows, wide[LAST]), half),
                pltpu.VMEM((rows, wide[LAST]), half),
                swapped,
                swapped,
                pltpu.VMEM((rows, hid), half),
                pltpu.VMEM((rows, own_hid), half),
                pltpu.SemaphoreType.DMA((5,)),
                pltpu.SemaphoreType.DMA((2, blocks)),
                pltpu.SemaphoreType.DMA((2, blocks)),
                pltpu.SemaphoreType.DMA((15,)),
                pltpu.SemaphoreType.DMA((15,)),
                pltpu.SemaphoreType.DMA((count, deepest)),
                pltpu.SemaphoreType.DMA((count, deepest)),
                pltpu.VMEM((1, LANES), single),
                pltpu.VMEM((n_dp * n_mp - 1, 1, LANES), single),
                pltpu.SemaphoreType.DMA((2,)),
            ]
        ),
        compiler_params=pltpu.CompilerParams(
            collective_id=0, has_side_effects=True, vmem_limit_bytes=60 * 1024 * 1024
        ),
    )(counts, *loads)
    finals = (
        (long[FIRST] // n_dp, in_width),
        (long[MIDDLE] // n_dp, own_hid),
        (long[LAST] // n_dp, own_width),
    )
    first, middle, last = pl.pallas_call(
        scale_kernel,
        out_shape=[jax.ShapeDtypeStruct(s, single) for s in finals],
        in_specs=[pl.BlockSpec(memory_space=pltpu.VMEM)] * 4,
        out_specs=[pl.BlockSpec(memory_space=pltpu.VMEM)] * 3,
    )(raws[3], *raws[:3])
    return first.T, middle.T, last


def solution(mesh):
    return jax.shard_map(
        functools.partial(per_device, (mesh.shape["dp"], mesh.shape["mp"])),
        mesh=mesh,
        in_specs=(
            P("dp", None),
            P("dp", None),
            P("dp"),
            P(None, "mp"),
            P("mp", None),
            P(None, "mp"),
        ),
        out_specs=(P(None, ("mp", "dp")), P("mp", "dp"), P("dp", "mp")),
        check_vma=False,
    )
```

```python
import functools
import math

import jax
import jax.numpy as jnp
from jax import lax
from jax.experimental import pallas as pl
from jax.experimental.pallas import tpu as pltpu
from jax.sharding import PartitionSpec as P

BLOCK = 128
LANES = 128
MESH = pl.DeviceIdType.MESH
FIRST, MIDDLE, LAST = 0, 1, 2
NT = (((1,), (1,)), ((), ()))


def silu_slope(pre_act):
    sigmoid_of = jax.nn.sigmoid(pre_act)
    return sigmoid_of * (1.0 + pre_act * (1.0 - sigmoid_of))


def pad_to(size, step):
    return -(-size // step) * step


SHARED = {FIRST: (0, 1), MIDDLE: (2,), LAST: (2,)}
PIECES = (
    (LAST, (0, 1), 1, 25.3, (30.1, 35.2, 50)),
    (LAST, (1, 0), 1, 25.4, (30.2, 35.3, 50.1)),
    (LAST, (0, 1), 2, 25.5, (34.2, 38.2, 53)),
    (LAST, (1, 0), 2, 25.6, (34.3, 38.3, 53.1)),
    (FIRST, (2,), 5, 18.8, (27.8, 48)),
    (FIRST, (2,), 5, 25.9, (34.6, 49)),
    (FIRST, (2,), 5, 27.8, (37.5, 51)),
    (FIRST, (2,), 6, 29.6, (40.4, 52)),
    (MIDDLE, (1, 0), 1, 33.6, (37.4, 43.3, 54)),
    (MIDDLE, (0, 1), 1, 33.7, (37.41, 43.4, 54.1)),
    (MIDDLE, (1, 0), 2, 34.5, (42.3, 46.2, 55)),
    (MIDDLE, (0, 1), 2, 34.6, (42.4, 46.3, 55.1)),
)


def pieces_of(n_dp, wide):
    total = n_dp.bit_length() - 1
    out = []
    for which in (LAST, FIRST, MIDDLE):
        mine = [piece for piece in PIECES if piece[0] == which]
        tiles, parts = wide[which] // LANES, [piece[2] for piece in mine]
        bounds = [
            round(tiles * sum(parts[:i]) / sum(parts)) * LANES for i in range(len(mine) + 1)
        ]
        for i, (_, head, _, when, keys) in enumerate(mine):
            tail = [b for b in range(total) if b not in SHARED[which] + head]
            bits = head + tuple(tail)
            more = len(bits) - len(keys)
            keys = keys[:-1] + tuple(keys[-2] + 7 * (j + 1) for j in range(more)) + (keys[-1] + 7 * more,)
            out.append((which, bounds[i], bounds[i + 1] - bounds[i], bits, when, keys))
    return out


def step_kernel(dims, params, pieces, stage_shapes, *refs):
    n_dp, n_mp = dims
    count = len(pieces)
    counts, loads, outs, scale_out = refs[0], refs[1:6], refs[6:9], refs[9]
    refs = refs[10:]
    held, got = [], []
    for group in (held, got):
        for shapes in stage_shapes:
            group.append(refs[: len(shapes)])
            refs = refs[len(shapes) :]
    finals, refs = refs[:count], refs[count:]
    belief_t, target_t, w_first, w_middle, w_last_t = refs[:5]
    parts_t, near_t = refs[5:8], refs[8:11]
    (
        belief, near_belief, pre1, act1, near_act1, part2, other2, pre2, act2, slope_out, near_out,
        part_back, other_back, slope2, slope1, load_sems, swap_send, swap_got, share_send, share_got,
        sends, gots, leave_sems, sq_send, sq_got, sq_sems,
    ) = refs[11:]

    in_width, own_hid = w_first.shape
    own_width, hid = w_last_t.shape
    rows = belief.shape[0]
    blocks = part2.shape[0]
    block = hid // blocks

    landing = (belief_t, target_t, w_first, w_middle, w_last_t)
    arrivals = [
        pltpu.make_async_copy(src, dst, load_sems.at[i])
        for i, (src, dst) in enumerate(zip(loads, landing))
    ]
    arrivals[0].start()

    dp, mp = lax.axis_index("dp"), lax.axis_index("mp")
    me = dp * n_mp + mp
    total = n_dp * n_mp

    def side(bit):
        return (dp // (1 << bit)) % 2

    def peer(bit):
        return (dp + (1 - 2 * side(bit)) * (1 << bit), mp)

    sibling = (dp, 1 - mp)
    x, y = (side(bit) for bit in SHARED[FIRST])
    x_peer, y_peer = (peer(bit) for bit in SHARED[FIRST])
    diagonal = (x_peer[0] + y_peer[0] - dp, mp)
    (low,) = SHARED[MIDDLE]
    z, z_peer = side(low), peer(low)
    bits = n_dp.bit_length() - 1
    partners = [sibling, diagonal] + [peer(bit) for bit in range(bits)]
    barrier = pltpu.get_barrier_semaphore()
    for partner in partners:
        pl.semaphore_signal(barrier, inc=1, device_id=partner, device_id_type=MESH)
    for i in (2, 3, 4, 1):
        arrivals[i].start()

    def remote(src, dst, sems, k, goal):
        return pltpu.make_async_remote_copy(
            src, dst, sems[0].at[k], sems[1].at[k], device_id=goal, device_id_type=MESH
        )

    share = functools.partial(remote, sems=(share_send, share_got))
    own_shares = 9
    my_rows = pl.ds(pl.multiple_of(mp * (rows // 2), rows // 2), rows // 2)
    relay_goal = (jnp.where(mp == 0, y_peer[0], x_peer[0]), mp)
    bands = [pl.ds(piece[1], piece[2]) for piece in pieces if piece[0] == FIRST]
    nears = []
    for i, goal in enumerate((x_peer, y_peer)):
        nears.append([
            share(
                belief.at[my_rows, band], near_belief.at[i, my_rows, band],
                k=own_shares + 6 * c + i, goal=goal,
            )
            for c, band in enumerate(bands)
        ])
    relays = [
        share(
            near_belief.at[mp, my_rows, band], near_belief.at[2, my_rows, band],
            k=own_shares + 6 * c + 2, goal=relay_goal,
        )
        for c, band in enumerate(bands)
    ]
    passes = [
        [
            share(
                near_belief.at[i, my_rows, band], near_belief.at[i, my_rows, band],
                k=own_shares + 6 * c + 3 + i, goal=sibling,
            )
            for i in range(3)
        ]
        for c, band in enumerate(bands)
    ]
    slopes = [
        share(parts_t[FIRST].at[at], near_t[FIRST].at[i], k=i, goal=goal)
        for i, (at, goal) in enumerate(
            (((1 - x, y), x_peer), ((x, 1 - y), y_peer), ((1 - x, 1 - y), diagonal))
        )
    ]
    send_act1 = share(act1, near_act1, k=3, goal=z_peer)
    send_act2 = share(parts_t[LAST].at[1 - z, mp], near_t[LAST].at[mp], k=4, goal=z_peer)
    send_out = share(slope_out, near_out, k=5, goal=z_peer)
    send_slope2 = share(parts_t[MIDDLE].at[1 - z, mp], near_t[MIDDLE].at[mp], k=6, goal=z_peer)
    pass_act2 = share(near_t[LAST].at[mp], near_t[LAST].at[mp], k=7, goal=sibling)
    pass_slope2 = share(near_t[MIDDLE].at[mp], near_t[MIDDLE].at[mp], k=8, goal=sibling)

    def swap(way, part, other, i):
        return pltpu.make_async_remote_copy(
            part.at[i], other.at[i], swap_send.at[way, i], swap_got.at[way, i],
            device_id=sibling, device_id_type=MESH,
        )

    def transpose_parts(which, source, width):
        order = SHARED[which] + tuple(b for b in range(bits) if b not in SHARED[which])
        r = width // n_dp
        step = math.lcm(r, LANES)
        for start in range(0, width, step):
            value = source[:, start : start + step].T
            for d in range(start // r, (start + step) // r):
                where = [(d >> bit) & 1 for bit in order]
                at = 0
                for bit in where[2:]:
                    at = 2 * at + bit
                parts_t[which][where[0], where[1], at * r : (at + 1) * r, :] = value[
                    d * r - start : (d + 1) * r - start
                ]

    def leave(p):
        which, start, width = pieces[p][:3]
        return pltpu.make_async_copy(
            finals[p], outs[which].at[:, pl.ds(start, width)], leave_sems.at[p]
        )

    def dot(left, right):
        return jnp.dot(left, right, preferred_element_type=jnp.float32)

    def first_grad(p):
        start, width = pieces[p][1:3]
        cols = slice(start, start + width)
        value = dot(parts_t[FIRST][x, y], belief[:, cols])
        for i in range(3):
            value = value + dot(near_t[FIRST][i], near_belief[i, :, cols])
        h = value.shape[0] // 2
        store(p, 0, 0, value[:h])
        store(p, 0, 1, value[h:])
        exchange(p, 0).start()

    rights = {MIDDLE: (act1, near_act1), LAST: (slope_out, near_out)}

    def half_grad(p, half):
        which, start, width, order, _, _ = pieces[p]
        own, near = rights[which]
        cols = slice(start, start + width)
        value = dot(parts_t[which][z, half], own[:, cols]) + dot(near_t[which][half], near[:, cols])
        if order[0] == 0:
            store(p, 0, half, value)
        else:
            h = value.shape[0] // 2
            held[p][0][0, half] = value[:h].astype(jnp.bfloat16)
            held[p][0][1, half] = value[h:].astype(jnp.bfloat16)

    def grad(p):
        if pieces[p][0] == FIRST:
            first_grad(p)
        elif pieces[p][3][0] == 0:
            half_grad(p, 1 - x)
            exchange(p, 0).start()
            half_grad(p, x)
        else:
            half_grad(p, 0)
            half_grad(p, 1)
            exchange(p, 0).start()

    def stages_of(p):
        return len(pieces[p][3])

    def store(p, k, half, value):
        ref = held[p][k]
        if k == stages_of(p) - 1:
            ref[half] = value.astype(jnp.bfloat16)
            return
        h = value.shape[0] // 2
        ref[half, 0] = value[:h].astype(jnp.bfloat16)
        ref[half, 1] = value[h:].astype(jnp.bfloat16)

    def exchange(p, k):
        bit = pieces[p][3][k]
        return pltpu.make_async_remote_copy(
            held[p][k].at[1 - side(bit)], got[p][k], sends.at[p, k], gots.at[p, k],
            device_id=peer(bit), device_id_type=MESH,
        )

    def turn(got_first, then):
        for copy in got_first:
            copy.wait_recv()
        for copy in then:
            copy.start()

    def hand_on(c):
        turn((nears[0][c], nears[1][c]), (relays[c], passes[c][0], passes[c][1]))

    arrivals[0].wait()
    for start in range(0, belief.shape[1], LANES * 3):
        value = belief_t[start : min(start + LANES * 3, in_width), :]
        if value.shape[0] < LANES * 3:
            value = jnp.concatenate(
                [value, jnp.zeros((LANES * 3 - value.shape[0], rows), jnp.bfloat16)], axis=0
            )
        belief[:, start : start + LANES * 3] = value.T
    pl.semaphore_wait(barrier, len(partners))
    early = len(bands) - 1
    for c in range(early):
        nears[0][c].start()
        nears[1][c].start()
    arrivals[2].wait()
    for c in range(0, own_hid, 256):
        value = jnp.dot(
            belief[:, :in_width], w_first[:, c : c + 256], preferred_element_type=jnp.float32
        )
        pre1[:, c : c + 256] = value
        act1[:, c : c + 256] = jax.nn.silu(value).astype(jnp.bfloat16)
    send_act1.start()
    arrivals[3].wait()
    for i in range(blocks):
        part2[i] = jnp.dot(
            act1[...], w_middle[:, i * block : (i + 1) * block],
            preferred_element_type=jnp.float32,
        )
        swap(0, part2, other2, i).start()
    arrivals[1].wait()
    arrivals[4].wait()
    row = lax.broadcasted_iota(jnp.int32, (rows, 1), 0)
    limit = jnp.full((rows, 1), counts[0], jnp.int32)
    for b in range(1, rows // BLOCK):
        limit = jnp.where(row >= b * BLOCK, counts[b] + b * BLOCK, limit)
    live = jnp.where(row < limit, 1.0, 0.0)
    target = target_t[...].T
    wanted = target[:, :own_width].astype(jnp.float32)
    for m in range(1, n_mp):
        wanted = jnp.where(
            mp == m, target[:, m * own_width : (m + 1) * own_width].astype(jnp.float32), wanted
        )
    for i in range(blocks):
        cols = slice(i * block, (i + 1) * block)
        swap(0, part2, other2, i).wait_recv()
        value = part2[i] + other2[i]
        pre2[:, cols] = value
        act2[:, cols] = jax.nn.silu(value).astype(jnp.bfloat16)
    transpose_parts(LAST, act2, hid)
    send_act2.start()
    predicted = lax.dot_general(act2[...], w_last_t[...], NT, preferred_element_type=jnp.float32)
    value = jnp.clip(predicted - wanted, -1.0, 1.0) * live
    slope_out[...] = jnp.concatenate(
        [value, jnp.zeros((rows, slope_out.shape[1] - own_width), jnp.float32)], axis=1
    ).astype(jnp.bfloat16)
    send_out.start()
    hand_on(0)

    for i in range(blocks):
        part_back[i] = jnp.dot(
            slope_out[:, :own_width], w_last_t[:, i * block : (i + 1) * block],
            preferred_element_type=jnp.float32,
        )
        swap(1, part_back, other_back, i).start()
    for i in range(blocks):
        cols = slice(i * block, (i + 1) * block)
        swap(1, part_back, other_back, i).wait_recv()
        value = (part_back[i] + other_back[i]) * silu_slope(pre2[:, cols])
        slope2[:, cols] = value.astype(jnp.bfloat16)
    transpose_parts(MIDDLE, slope2, hid)
    for c in range(0, own_hid, 256):
        back = lax.dot_general(
            slope2[...], w_middle[c : c + 256, :], NT, preferred_element_type=jnp.float32
        )
        slope1[:, c : c + 256] = (back * silu_slope(pre1[:, c : c + 256])).astype(jnp.bfloat16)
    transpose_parts(FIRST, slope1, own_hid)
    for copy in slopes:
        copy.start()
    for c in range(early, len(bands)):
        nears[0][c].start()
        nears[1][c].start()

    def step(p, k):
        mine = side(pieces[p][3][k])
        exchange(p, k).wait_recv()
        for h in range(2):
            value = held[p][k][mine, h].astype(jnp.float32) + got[p][k][h].astype(jnp.float32)
            store(p, k + 1, h, value)
        exchange(p, k + 1).start()

    def finish(p, k):
        mine = side(pieces[p][3][k])
        exchange(p, k).wait_recv()
        value = held[p][k][mine].astype(jnp.float32) + got[p][k][...].astype(jnp.float32)
        finals[p][...] = value
        leave(p).start()
        across = jnp.sum(value * value, axis=0, keepdims=True)
        for start in range(0, value.shape[1], LANES):
            squares.append(across[:, start : start + LANES])

    squares = []
    actions = [
        (15, turn, ([relays[0]], [passes[0][2]])),
        (16.8, turn, ([send_act2], [pass_act2])),
        (18.7, turn, (slopes + passes[0], [])),
        (18.9, turn, ([], [send_slope2])),
        (25.2, turn, ([pass_act2, send_out], [])),
        (31.9, turn, ([send_slope2], [pass_slope2])),
        (33.5, turn, ([send_act1, pass_slope2], [])),
    ]
    for c in range(1, len(bands)):
        seen = 12.1 + 0.6 * c if c < early else 22.4
        actions.append((seen, hand_on, (c,)))
        actions.append((22.2 + 1.9 * c, turn, ([relays[c]], [passes[c][2]])))
        actions.append((23.9 + 1.9 * c, turn, (passes[c], [])))
    for p in range(count):
        actions.append((pieces[p][4], grad, (p,)))
        for k in range(stages_of(p)):
            does = step if k < stages_of(p) - 1 else finish
            actions.append((pieces[p][5][k], does, (p, k)))
    for _, does, what in sorted(actions, key=lambda action: action[0]):
        does(*what)
    squares = jnp.sum(sum(squares[1:], squares[0]), axis=1, keepdims=True)

    sq_send[...] = jnp.broadcast_to(squares, sq_send.shape)

    def square_copy(j):
        other = lax.rem(me + j, total)
        return pltpu.make_async_remote_copy(
            sq_send, sq_got.at[j - 1], sq_sems.at[0], sq_sems.at[1],
            device_id=(other // n_mp, other % n_mp), device_id_type=MESH,
        )

    def tell(j, _):
        square_copy(j).start()
        return 0

    lax.fori_loop(1, total, tell, 0)
    for i in range(blocks):
        swap(0, part2, other2, i).wait_send()
        swap(1, part_back, other_back, i).wait_send()
    for copy in (
        *nears[0], *nears[1], *relays, *sum(passes, []), *slopes,
        send_act1, send_act2, send_out, send_slope2, pass_act2, pass_slope2,
    ):
        copy.wait_send()
    for p in range(count):
        for k in range(stages_of(p)):
            exchange(p, k).wait_send()
        leave(p).wait()
    pltpu.make_async_copy(sq_got, sq_got, sq_sems.at[1]).wait()
    everyone = squares + jnp.sum(sq_got[...], axis=0)
    scale_out[...] = jnp.broadcast_to(lax.rsqrt(everyone / params + 1e-06), scale_out.shape)
    pltpu.make_async_copy(sq_got, sq_got, sq_sems.at[0]).wait()


def scale_kernel(scale, *refs):
    factor = scale[0:1, 0:1]
    for raw, out in zip(refs[:3], refs[3:]):
        out[...] = raw[:, : out.shape[1]] * factor


def per_device(dims, belief, target_value, counts, w_first, w_middle, w_last):
    n_dp, n_mp = dims
    blocks = 3
    rows, (in_width, own_hid) = belief.shape[0], w_first.shape
    hid, own_width = w_last.shape
    params = float(n_mp * (w_first.size + w_middle.size + w_last.size))
    long = {FIRST: own_hid, MIDDLE: hid, LAST: hid}
    wide = {
        FIRST: pad_to(in_width, LANES),
        MIDDLE: pad_to(own_hid, LANES),
        LAST: pad_to(own_width, LANES),
    }
    layers = (FIRST, MIDDLE, LAST)
    pieces = pieces_of(n_dp, wide)
    half, single = jnp.bfloat16, jnp.float32

    def stage_shapes(piece):
        stages = len(piece[3])
        for k in range(stages):
            r = long[piece[0]] >> (len(SHARED[piece[0]]) + k + 1)
            yield (2, r, piece[2]) if k == stages - 1 else (2, 2, r // 2, piece[2])

    shapes = [list(stage_shapes(piece)) for piece in pieces]
    shares = 9 + 6 * sum(piece[0] == FIRST for piece in pieces)
    deepest = max(len(stages) for stages in shapes)
    loads = (belief.T, target_value.T, w_first, w_middle, w_last.T)
    swapped = pltpu.VMEM((blocks, rows, hid // blocks), single)
    count = len(pieces)
    raws = pl.pallas_call(
        functools.partial(step_kernel, dims, params, pieces, shapes),
        out_shape=[
            jax.ShapeDtypeStruct((long[w] // n_dp, wide[w]), single) for w in layers
        ] + [jax.ShapeDtypeStruct((8, LANES), single)],
        in_specs=[pl.BlockSpec(memory_space=pltpu.SMEM)]
        + [pl.BlockSpec(memory_space=pl.ANY)] * 5,
        out_specs=[pl.BlockSpec(memory_space=pl.ANY)] * 3
        + [pl.BlockSpec(memory_space=pltpu.VMEM)],
        scratch_shapes=(
            [pltpu.VMEM(s, half) for stages in shapes for s in stages]
            + [pltpu.VMEM(s[1:], half) for stages in shapes for s in stages]
            + [pltpu.VMEM(stages[-1][1:], single) for stages in shapes]
            + [
                pltpu.VMEM((in_width, rows), half),
                pltpu.VMEM((n_mp * own_width, rows), half),
                pltpu.VMEM(w_first.shape, half),
                pltpu.VMEM(w_middle.shape, half),
                pltpu.VMEM((own_width, hid), half),
            ]
            + [pltpu.VMEM((2, 2, long[w] // 4, rows), half) for w in layers]
            + [pltpu.VMEM((3 if w == FIRST else 2, long[w] // 4, rows), half) for w in layers]
            + [
                pltpu.VMEM((rows, wide[FIRST]), half),
                pltpu.VMEM((3, rows, wide[FIRST]), half),
                pltpu.VMEM((rows, own_hid), single),
                pltpu.VMEM((rows, own_hid), half),
                pltpu.VMEM((rows, own_hid), half),
                swapped,
                swapped,
                pltpu.VMEM((rows, hid), single),
                pltpu.VMEM((rows, hid), half),
                pltpu.VMEM((rows, wide[LAST]), half),
                pltpu.VMEM((rows, wide[LAST]), half),
                swapped,
                swapped,
                pltpu.VMEM((rows, hid), half),
                pltpu.VMEM((rows, own_hid), half),
                pltpu.SemaphoreType.DMA((5,)),
                pltpu.SemaphoreType.DMA((2, blocks)),
                pltpu.SemaphoreType.DMA((2, blocks)),
                pltpu.SemaphoreType.DMA((shares,)),
                pltpu.SemaphoreType.DMA((shares,)),
                pltpu.SemaphoreType.DMA((count, deepest)),
                pltpu.SemaphoreType.DMA((count, deepest)),
                pltpu.SemaphoreType.DMA((count,)),
                pltpu.VMEM((1, LANES), single),
                pltpu.VMEM((n_dp * n_mp - 1, 1, LANES), single),
                pltpu.SemaphoreType.DMA((2,)),
            ]
        ),
        compiler_params=pltpu.CompilerParams(
            collective_id=0, has_side_effects=True, vmem_limit_bytes=60 * 1024 * 1024
        ),
    )(counts, *loads)
    ends = (
        (long[FIRST] // n_dp, in_width),
        (long[MIDDLE] // n_dp, own_hid),
        (long[LAST] // n_dp, own_width),
    )
    first, middle, last = pl.pallas_call(
        scale_kernel,
        out_shape=[jax.ShapeDtypeStruct(s, single) for s in ends],
        in_specs=[pl.BlockSpec(memory_space=pltpu.VMEM)] * 4,
        out_specs=[pl.BlockSpec(memory_space=pltpu.VMEM)] * 3,
    )(raws[3], *raws[:3])
    return first.T, middle.T, last


def solution(mesh):
    return jax.shard_map(
        functools.partial(per_device, (mesh.shape["dp"], mesh.shape["mp"])),
        mesh=mesh,
        in_specs=(
            P("dp", None),
            P("dp", None),
            P("dp"),
            P(None, "mp"),
            P("mp", None),
            P(None, "mp"),
        ),
        out_specs=(P(None, ("mp", "dp")), P("mp", "dp"), P("dp", "mp")),
        check_vma=False,
    )
```

```python
import functools
import math

import jax
import jax.numpy as jnp
from jax import lax
from jax.experimental import pallas as pl
from jax.experimental.pallas import tpu as pltpu
from jax.sharding import PartitionSpec as P

BLOCK = 128
LANES = 128
MESH = pl.DeviceIdType.MESH
FIRST, MIDDLE, LAST = 0, 1, 2
NT = (((1,), (1,)), ((), ()))


def silu_slope(pre_act):
    sigmoid_of = jax.nn.sigmoid(pre_act)
    return sigmoid_of * (1.0 + pre_act * (1.0 - sigmoid_of))


def pad_to(size, step):
    return -(-size // step) * step


SHARED = {FIRST: (0, 1), MIDDLE: (2,), LAST: (3,)}
PIECES = (
    (LAST, (0, 1), 1, 34.4, (38.2, 43.4, 53)),
    (LAST, (1, 0), 1, 34.5, (38.3, 43.5, 53.1)),
    (LAST, (0, 1), 2, 34.6, (42.4, 46.2, 54)),
    (LAST, (1, 0), 2, 34.7, (42.5, 46.3, 54.1)),
    (FIRST, (2,), 5, 18.8, (36.2, 50)),
    (FIRST, (2,), 5, 25.9, (38.7, 50.1)),
    (FIRST, (2,), 5, 27.8, (41.4, 51)),
    (FIRST, (2,), 6, 29.6, (44.6, 52)),
    (MIDDLE, (1, 0), 1, 27, (30.8, 36, 49)),
    (MIDDLE, (0, 1), 1, 27.1, (30.9, 36.1, 49.1)),
    (MIDDLE, (1, 0), 2, 27.2, (35, 38.8, 50.5)),
    (MIDDLE, (0, 1), 2, 27.3, (35.1, 38.9, 50.6)),
)


def pieces_of(n_dp, wide):
    total = n_dp.bit_length() - 1
    out = []
    for which in (LAST, FIRST, MIDDLE):
        mine = [piece for piece in PIECES if piece[0] == which]
        tiles, parts = wide[which] // LANES, [piece[2] for piece in mine]
        bounds = [
            round(tiles * sum(parts[:i]) / sum(parts)) * LANES for i in range(len(mine) + 1)
        ]
        for i, (_, head, _, when, keys) in enumerate(mine):
            tail = [b for b in range(total) if b not in SHARED[which] + head]
            bits = head + tuple(tail)
            more = len(bits) - len(keys)
            keys = keys[:-1] + tuple(keys[-2] + 7 * (j + 1) for j in range(more)) + (keys[-1] + 7 * more,)
            out.append((which, bounds[i], bounds[i + 1] - bounds[i], bits, when, keys))
    return out


def step_kernel(dims, params, pieces, stage_shapes, *refs):
    n_dp, n_mp = dims
    count = len(pieces)
    counts, loads, outs, scale_out = refs[0], refs[1:6], refs[6:9], refs[9]
    refs = refs[10:]
    held, got = [], []
    for group in (held, got):
        for shapes in stage_shapes:
            group.append(refs[: len(shapes)])
            refs = refs[len(shapes) :]
    finals, refs = refs[:count], refs[count:]
    belief_t, target_t, w_first, w_middle, w_last_t = refs[:5]
    parts_t, near_t = refs[5:8], refs[8:11]
    (
        belief, near_belief, pre1, act1, near_act1, part2, other2, pre2, act2, slope_out, near_out,
        part_back, other_back, slope2, slope1, load_sems, swap_send, swap_got, share_send, share_got,
        sends, gots, leave_sems, sq_send, sq_got, sq_sems,
    ) = refs[11:]

    in_width, own_hid = w_first.shape
    own_width, hid = w_last_t.shape
    rows = belief.shape[0]
    blocks = part2.shape[0]
    block = hid // blocks

    landing = (belief_t, target_t, w_first, w_middle, w_last_t)
    arrivals = [
        pltpu.make_async_copy(src, dst, load_sems.at[i])
        for i, (src, dst) in enumerate(zip(loads, landing))
    ]
    arrivals[0].start()

    dp, mp = lax.axis_index("dp"), lax.axis_index("mp")
    me = dp * n_mp + mp
    total = n_dp * n_mp

    def side(bit):
        return (dp // (1 << bit)) % 2

    def peer(bit):
        return (dp + (1 - 2 * side(bit)) * (1 << bit), mp)

    sibling = (dp, 1 - mp)
    x, y = (side(bit) for bit in SHARED[FIRST])
    x_peer, y_peer = (peer(bit) for bit in SHARED[FIRST])
    diagonal = (x_peer[0] + y_peer[0] - dp, mp)
    pair_side = {which: side(SHARED[which][0]) for which in (MIDDLE, LAST)}
    pair_peer = {which: peer(SHARED[which][0]) for which in (MIDDLE, LAST)}
    bits = n_dp.bit_length() - 1
    partners = [sibling, diagonal] + [peer(bit) for bit in range(bits)]
    barrier = pltpu.get_barrier_semaphore()
    for partner in partners:
        pl.semaphore_signal(barrier, inc=1, device_id=partner, device_id_type=MESH)
    for i in (2, 3, 4, 1):
        arrivals[i].start()

    def remote(src, dst, sems, k, goal):
        return pltpu.make_async_remote_copy(
            src, dst, sems[0].at[k], sems[1].at[k], device_id=goal, device_id_type=MESH
        )

    share = functools.partial(remote, sems=(share_send, share_got))
    own_shares = 9
    my_rows = pl.ds(pl.multiple_of(mp * (rows // 2), rows // 2), rows // 2)
    relay_goal = (jnp.where(mp == 0, y_peer[0], x_peer[0]), mp)
    bands = [pl.ds(piece[1], piece[2]) for piece in pieces if piece[0] == FIRST]
    nears = []
    for i, goal in enumerate((x_peer, y_peer)):
        nears.append([
            share(
                belief.at[my_rows, band], near_belief.at[i, my_rows, band],
                k=own_shares + 6 * c + i, goal=goal,
            )
            for c, band in enumerate(bands)
        ])
    relays = [
        share(
            near_belief.at[mp, my_rows, band], near_belief.at[2, my_rows, band],
            k=own_shares + 6 * c + 2, goal=relay_goal,
        )
        for c, band in enumerate(bands)
    ]
    passes = [
        [
            share(
                near_belief.at[i, my_rows, band], near_belief.at[i, my_rows, band],
                k=own_shares + 6 * c + 3 + i, goal=sibling,
            )
            for i in range(3)
        ]
        for c, band in enumerate(bands)
    ]
    slopes = [
        share(parts_t[FIRST].at[at], near_t[FIRST].at[i], k=i, goal=goal)
        for i, (at, goal) in enumerate(
            (((1 - x, y), x_peer), ((x, 1 - y), y_peer), ((1 - x, 1 - y), diagonal))
        )
    ]
    send_act1 = share(act1, near_act1, k=3, goal=pair_peer[MIDDLE])
    send_act2 = share(
        parts_t[LAST].at[1 - pair_side[LAST], mp], near_t[LAST].at[mp], k=4, goal=pair_peer[LAST]
    )
    send_out = share(slope_out, near_out, k=5, goal=pair_peer[LAST])
    send_slope2 = share(
        parts_t[MIDDLE].at[1 - pair_side[MIDDLE], mp], near_t[MIDDLE].at[mp], k=6,
        goal=pair_peer[MIDDLE],
    )
    pass_act2 = share(near_t[LAST].at[mp], near_t[LAST].at[mp], k=7, goal=sibling)
    pass_slope2 = share(near_t[MIDDLE].at[mp], near_t[MIDDLE].at[mp], k=8, goal=sibling)

    def swap(way, part, other, i):
        return pltpu.make_async_remote_copy(
            part.at[i], other.at[i], swap_send.at[way, i], swap_got.at[way, i],
            device_id=sibling, device_id_type=MESH,
        )

    def transpose_parts(which, source, width):
        order = SHARED[which] + tuple(b for b in range(bits) if b not in SHARED[which])
        r = width // n_dp
        step = math.lcm(r, LANES)
        for start in range(0, width, step):
            value = source[:, start : start + step].T
            for d in range(start // r, (start + step) // r):
                where = [(d >> bit) & 1 for bit in order]
                at = 0
                for bit in where[2:]:
                    at = 2 * at + bit
                parts_t[which][where[0], where[1], at * r : (at + 1) * r, :] = value[
                    d * r - start : (d + 1) * r - start
                ]

    def leave(p):
        which, start, width = pieces[p][:3]
        return pltpu.make_async_copy(
            finals[p], outs[which].at[:, pl.ds(start, width)], leave_sems.at[p]
        )

    def dot(left, right):
        return jnp.dot(left, right, preferred_element_type=jnp.float32)

    def first_grad(p):
        start, width = pieces[p][1:3]
        cols = slice(start, start + width)
        value = dot(parts_t[FIRST][x, y], belief[:, cols])
        for i in range(3):
            value = value + dot(near_t[FIRST][i], near_belief[i, :, cols])
        h = value.shape[0] // 2
        store(p, 0, 0, value[:h])
        store(p, 0, 1, value[h:])
        exchange(p, 0).start()

    rights = {MIDDLE: (act1, near_act1), LAST: (slope_out, near_out)}

    def half_grad(p, half):
        which, start, width, order, _, _ = pieces[p]
        own, near = rights[which]
        cols = slice(start, start + width)
        value = dot(parts_t[which][pair_side[which], half], own[:, cols])
        value = value + dot(near_t[which][half], near[:, cols])
        if order[0] == 0:
            store(p, 0, half, value)
        else:
            h = value.shape[0] // 2
            held[p][0][0, half] = value[:h].astype(jnp.bfloat16)
            held[p][0][1, half] = value[h:].astype(jnp.bfloat16)

    def grad(p):
        if pieces[p][0] == FIRST:
            first_grad(p)
        elif pieces[p][3][0] == 0:
            half_grad(p, 1 - x)
            exchange(p, 0).start()
            half_grad(p, x)
        else:
            half_grad(p, 0)
            half_grad(p, 1)
            exchange(p, 0).start()

    def stages_of(p):
        return len(pieces[p][3])

    def store(p, k, half, value):
        ref = held[p][k]
        if k == stages_of(p) - 1:
            ref[half] = value.astype(jnp.bfloat16)
            return
        h = value.shape[0] // 2
        ref[half, 0] = value[:h].astype(jnp.bfloat16)
        ref[half, 1] = value[h:].astype(jnp.bfloat16)

    def exchange(p, k):
        bit = pieces[p][3][k]
        return pltpu.make_async_remote_copy(
            held[p][k].at[1 - side(bit)], got[p][k], sends.at[p, k], gots.at[p, k],
            device_id=peer(bit), device_id_type=MESH,
        )

    def turn(got_first, then):
        for copy in got_first:
            copy.wait_recv()
        for copy in then:
            copy.start()

    def hand_on(c):
        turn((nears[0][c], nears[1][c]), (relays[c], passes[c][0], passes[c][1]))

    arrivals[0].wait()
    for start in range(0, belief.shape[1], LANES * 3):
        value = belief_t[start : min(start + LANES * 3, in_width), :]
        if value.shape[0] < LANES * 3:
            value = jnp.concatenate(
                [value, jnp.zeros((LANES * 3 - value.shape[0], rows), jnp.bfloat16)], axis=0
            )
        belief[:, start : start + LANES * 3] = value.T
    pl.semaphore_wait(barrier, len(partners))
    early = len(bands) - 1
    for c in range(early):
        nears[0][c].start()
        nears[1][c].start()
    arrivals[2].wait()
    for c in range(0, own_hid, 256):
        value = jnp.dot(
            belief[:, :in_width], w_first[:, c : c + 256], preferred_element_type=jnp.float32
        )
        pre1[:, c : c + 256] = value
        act1[:, c : c + 256] = jax.nn.silu(value).astype(jnp.bfloat16)
    send_act1.start()
    arrivals[3].wait()
    for i in range(blocks):
        part2[i] = jnp.dot(
            act1[...], w_middle[:, i * block : (i + 1) * block],
            preferred_element_type=jnp.float32,
        )
        swap(0, part2, other2, i).start()
    arrivals[1].wait()
    arrivals[4].wait()
    row = lax.broadcasted_iota(jnp.int32, (rows, 1), 0)
    limit = jnp.full((rows, 1), counts[0], jnp.int32)
    for b in range(1, rows // BLOCK):
        limit = jnp.where(row >= b * BLOCK, counts[b] + b * BLOCK, limit)
    live = jnp.where(row < limit, 1.0, 0.0)
    target = target_t[...].T
    wanted = target[:, :own_width].astype(jnp.float32)
    for m in range(1, n_mp):
        wanted = jnp.where(
            mp == m, target[:, m * own_width : (m + 1) * own_width].astype(jnp.float32), wanted
        )
    for i in range(blocks):
        cols = slice(i * block, (i + 1) * block)
        swap(0, part2, other2, i).wait_recv()
        value = part2[i] + other2[i]
        pre2[:, cols] = value
        act2[:, cols] = jax.nn.silu(value).astype(jnp.bfloat16)
    transpose_parts(LAST, act2, hid)
    send_act2.start()
    predicted = lax.dot_general(act2[...], w_last_t[...], NT, preferred_element_type=jnp.float32)
    value = jnp.clip(predicted - wanted, -1.0, 1.0) * live
    slope_out[...] = jnp.concatenate(
        [value, jnp.zeros((rows, slope_out.shape[1] - own_width), jnp.float32)], axis=1
    ).astype(jnp.bfloat16)
    hand_on(0)

    for i in range(blocks):
        part_back[i] = jnp.dot(
            slope_out[:, :own_width], w_last_t[:, i * block : (i + 1) * block],
            preferred_element_type=jnp.float32,
        )
        swap(1, part_back, other_back, i).start()
    for i in range(blocks):
        cols = slice(i * block, (i + 1) * block)
        swap(1, part_back, other_back, i).wait_recv()
        value = (part_back[i] + other_back[i]) * silu_slope(pre2[:, cols])
        slope2[:, cols] = value.astype(jnp.bfloat16)
    transpose_parts(MIDDLE, slope2, hid)
    send_slope2.start()
    for c in range(0, own_hid, 256):
        back = lax.dot_general(
            slope2[...], w_middle[c : c + 256, :], NT, preferred_element_type=jnp.float32
        )
        slope1[:, c : c + 256] = (back * silu_slope(pre1[:, c : c + 256])).astype(jnp.bfloat16)
    transpose_parts(FIRST, slope1, own_hid)
    for copy in slopes:
        copy.start()
    for c in range(early, len(bands)):
        nears[0][c].start()
        nears[1][c].start()

    def step(p, k):
        mine = side(pieces[p][3][k])
        exchange(p, k).wait_recv()
        for h in range(2):
            value = held[p][k][mine, h].astype(jnp.float32) + got[p][k][h].astype(jnp.float32)
            store(p, k + 1, h, value)
        exchange(p, k + 1).start()

    def finish(p, k):
        mine = side(pieces[p][3][k])
        exchange(p, k).wait_recv()
        value = held[p][k][mine].astype(jnp.float32) + got[p][k][...].astype(jnp.float32)
        finals[p][...] = value
        leave(p).start()
        across = jnp.sum(value * value, axis=0, keepdims=True)
        for start in range(0, value.shape[1], LANES):
            squares.append(across[:, start : start + LANES])

    squares = []
    actions = [
        (15, turn, ([relays[0]], [passes[0][2]])),
        (18.7, turn, (slopes + passes[0], [])),
        (11.9, turn, ([], [send_out])),
        (21.8, turn, ([send_act2], [pass_act2])),
        (25.3, turn, ([send_slope2], [pass_slope2])),
        (26.9, turn, ([send_act1, pass_slope2], [])),
        (34.3, turn, ([pass_act2, send_out], [])),
    ]
    for c in range(1, len(bands)):
        seen = 12.1 + 0.6 * c if c < early else 22.4
        actions.append((seen, hand_on, (c,)))
        actions.append((22.2 + 1.9 * c, turn, ([relays[c]], [passes[c][2]])))
        actions.append((23.9 + 1.9 * c, turn, (passes[c], [])))
    for p in range(count):
        actions.append((pieces[p][4], grad, (p,)))
        for k in range(stages_of(p)):
            does = step if k < stages_of(p) - 1 else finish
            actions.append((pieces[p][5][k], does, (p, k)))
    for _, does, what in sorted(actions, key=lambda action: action[0]):
        does(*what)
    squares = jnp.sum(sum(squares[1:], squares[0]), axis=1, keepdims=True)

    sq_send[...] = jnp.broadcast_to(squares, sq_send.shape)

    def square_copy(j):
        other = lax.rem(me + j, total)
        return pltpu.make_async_remote_copy(
            sq_send, sq_got.at[j - 1], sq_sems.at[0], sq_sems.at[1],
            device_id=(other // n_mp, other % n_mp), device_id_type=MESH,
        )

    def tell(j, _):
        square_copy(j).start()
        return 0

    lax.fori_loop(1, total, tell, 0)
    for i in range(blocks):
        swap(0, part2, other2, i).wait_send()
        swap(1, part_back, other_back, i).wait_send()
    for copy in (
        *nears[0], *nears[1], *relays, *sum(passes, []), *slopes,
        send_act1, send_act2, send_out, send_slope2, pass_act2, pass_slope2,
    ):
        copy.wait_send()
    for p in range(count):
        for k in range(stages_of(p)):
            exchange(p, k).wait_send()
        leave(p).wait()
    pltpu.make_async_copy(sq_got, sq_got, sq_sems.at[1]).wait()
    everyone = squares + jnp.sum(sq_got[...], axis=0)
    scale_out[...] = jnp.broadcast_to(lax.rsqrt(everyone / params + 1e-06), scale_out.shape)
    pltpu.make_async_copy(sq_got, sq_got, sq_sems.at[0]).wait()


def scale_kernel(scale, *refs):
    factor = scale[0:1, 0:1]
    for raw, out in zip(refs[:3], refs[3:]):
        out[...] = raw[:, : out.shape[1]] * factor


def per_device(dims, belief, target_value, counts, w_first, w_middle, w_last):
    n_dp, n_mp = dims
    blocks = 3
    rows, (in_width, own_hid) = belief.shape[0], w_first.shape
    hid, own_width = w_last.shape
    params = float(n_mp * (w_first.size + w_middle.size + w_last.size))
    long = {FIRST: own_hid, MIDDLE: hid, LAST: hid}
    wide = {
        FIRST: pad_to(in_width, LANES),
        MIDDLE: pad_to(own_hid, LANES),
        LAST: pad_to(own_width, LANES),
    }
    layers = (FIRST, MIDDLE, LAST)
    pieces = pieces_of(n_dp, wide)
    half, single = jnp.bfloat16, jnp.float32

    def stage_shapes(piece):
        stages = len(piece[3])
        for k in range(stages):
            r = long[piece[0]] >> (len(SHARED[piece[0]]) + k + 1)
            yield (2, r, piece[2]) if k == stages - 1 else (2, 2, r // 2, piece[2])

    shapes = [list(stage_shapes(piece)) for piece in pieces]
    shares = 9 + 6 * sum(piece[0] == FIRST for piece in pieces)
    deepest = max(len(stages) for stages in shapes)
    loads = (belief.T, target_value.T, w_first, w_middle, w_last.T)
    swapped = pltpu.VMEM((blocks, rows, hid // blocks), single)
    count = len(pieces)
    raws = pl.pallas_call(
        functools.partial(step_kernel, dims, params, pieces, shapes),
        out_shape=[
            jax.ShapeDtypeStruct((long[w] // n_dp, wide[w]), single) for w in layers
        ] + [jax.ShapeDtypeStruct((8, LANES), single)],
        in_specs=[pl.BlockSpec(memory_space=pltpu.SMEM)]
        + [pl.BlockSpec(memory_space=pl.ANY)] * 5,
        out_specs=[pl.BlockSpec(memory_space=pl.ANY)] * 3
        + [pl.BlockSpec(memory_space=pltpu.VMEM)],
        scratch_shapes=(
            [pltpu.VMEM(s, half) for stages in shapes for s in stages]
            + [pltpu.VMEM(s[1:], half) for stages in shapes for s in stages]
            + [pltpu.VMEM(stages[-1][1:], single) for stages in shapes]
            + [
                pltpu.VMEM((in_width, rows), half),
                pltpu.VMEM((n_mp * own_width, rows), half),
                pltpu.VMEM(w_first.shape, half),
                pltpu.VMEM(w_middle.shape, half),
                pltpu.VMEM((own_width, hid), half),
            ]
            + [pltpu.VMEM((2, 2, long[w] // 4, rows), half) for w in layers]
            + [pltpu.VMEM((3 if w == FIRST else 2, long[w] // 4, rows), half) for w in layers]
            + [
                pltpu.VMEM((rows, wide[FIRST]), half),
                pltpu.VMEM((3, rows, wide[FIRST]), half),
                pltpu.VMEM((rows, own_hid), single),
                pltpu.VMEM((rows, own_hid), half),
                pltpu.VMEM((rows, own_hid), half),
                swapped,
                swapped,
                pltpu.VMEM((rows, hid), single),
                pltpu.VMEM((rows, hid), half),
                pltpu.VMEM((rows, wide[LAST]), half),
                pltpu.VMEM((rows, wide[LAST]), half),
                swapped,
                swapped,
                pltpu.VMEM((rows, hid), half),
                pltpu.VMEM((rows, own_hid), half),
                pltpu.SemaphoreType.DMA((5,)),
                pltpu.SemaphoreType.DMA((2, blocks)),
                pltpu.SemaphoreType.DMA((2, blocks)),
                pltpu.SemaphoreType.DMA((shares,)),
                pltpu.SemaphoreType.DMA((shares,)),
                pltpu.SemaphoreType.DMA((count, deepest)),
                pltpu.SemaphoreType.DMA((count, deepest)),
                pltpu.SemaphoreType.DMA((count,)),
                pltpu.VMEM((1, LANES), single),
                pltpu.VMEM((n_dp * n_mp - 1, 1, LANES), single),
                pltpu.SemaphoreType.DMA((2,)),
            ]
        ),
        compiler_params=pltpu.CompilerParams(
            collective_id=0, has_side_effects=True, vmem_limit_bytes=60 * 1024 * 1024
        ),
    )(counts, *loads)
    ends = (
        (long[FIRST] // n_dp, in_width),
        (long[MIDDLE] // n_dp, own_hid),
        (long[LAST] // n_dp, own_width),
    )
    first, middle, last = pl.pallas_call(
        scale_kernel,
        out_shape=[jax.ShapeDtypeStruct(s, single) for s in ends],
        in_specs=[pl.BlockSpec(memory_space=pltpu.VMEM)] * 4,
        out_specs=[pl.BlockSpec(memory_space=pltpu.VMEM)] * 3,
    )(raws[3], *raws[:3])
    return first.T, middle.T, last


def solution(mesh):
    return jax.shard_map(
        functools.partial(per_device, (mesh.shape["dp"], mesh.shape["mp"])),
        mesh=mesh,
        in_specs=(
            P("dp", None),
            P("dp", None),
            P("dp"),
            P(None, "mp"),
            P("mp", None),
            P(None, "mp"),
        ),
        out_specs=(P(None, ("mp", "dp")), P("mp", "dp"), P("dp", "mp")),
        check_vma=False,
    )
```

```python
import functools
import math

import jax
import jax.numpy as jnp
from jax import lax
from jax.experimental import pallas as pl
from jax.experimental.pallas import tpu as pltpu
from jax.sharding import PartitionSpec as P

BLOCK = 128
LANES = 128
MESH = pl.DeviceIdType.MESH
FIRST, MIDDLE, LAST = 0, 1, 2
NT = (((1,), (1,)), ((), ()))


def silu_slope(pre_act):
    sigmoid_of = jax.nn.sigmoid(pre_act)
    return sigmoid_of * (1.0 + pre_act * (1.0 - sigmoid_of))


def pad_to(size, step):
    return -(-size // step) * step


SHARED = {FIRST: (0, 1), MIDDLE: (2,), LAST: (3,)}
PIECES = (
    (LAST, (0, 1), 1, 34.4, (38.2, 43.4, 53)),
    (LAST, (1, 0), 1, 34.5, (38.3, 43.5, 53.1)),
    (LAST, (0, 1), 2, 34.6, (42.4, 46.2, 54)),
    (LAST, (1, 0), 2, 34.7, (42.5, 46.3, 54.1)),
    (FIRST, (2,), 5, 18.8, (36.2, 50)),
    (FIRST, (2,), 5, 25.9, (38.7, 50.1)),
    (FIRST, (2,), 5, 27.8, (41.4, 51)),
    (FIRST, (2,), 6, 29.6, (44.6, 52)),
    (MIDDLE, (1, 0), 1, 27, (30.8, 36, 49)),
    (MIDDLE, (0, 1), 1, 27.1, (30.9, 36.1, 49.1)),
    (MIDDLE, (1, 0), 2, 27.2, (35, 38.8, 50.5)),
    (MIDDLE, (0, 1), 2, 27.3, (35.1, 38.9, 50.6)),
)


def pieces_of(n_dp, wide):
    total = n_dp.bit_length() - 1
    out = []
    for which in (LAST, FIRST, MIDDLE):
        mine = [piece for piece in PIECES if piece[0] == which]
        tiles, parts = wide[which] // LANES, [piece[2] for piece in mine]
        bounds = [
            round(tiles * sum(parts[:i]) / sum(parts)) * LANES for i in range(len(mine) + 1)
        ]
        for i, (_, head, _, when, keys) in enumerate(mine):
            tail = [b for b in range(total) if b not in SHARED[which] + head]
            bits = head + tuple(tail)
            more = len(bits) - len(keys)
            keys = keys[:-1] + tuple(keys[-2] + 7 * (j + 1) for j in range(more)) + (keys[-1] + 7 * more,)
            out.append((which, bounds[i], bounds[i + 1] - bounds[i], bits, when, keys))
    return out


def step_kernel(dims, params, pieces, stage_shapes, *refs):
    n_dp, n_mp = dims
    count = len(pieces)
    counts, loads, outs, scale_out = refs[0], refs[1:6], refs[6:9], refs[9]
    refs = refs[10:]
    held, got = [], []
    for group in (held, got):
        for shapes in stage_shapes:
            group.append(refs[: len(shapes)])
            refs = refs[len(shapes) :]
    finals, refs = refs[:count], refs[count:]
    belief_t, target_t, w_first, w_middle, w_last_t = refs[:5]
    parts_t, near_t = refs[5:8], refs[8:11]
    (
        belief, near_belief, pre1, act1, near_act1, part2, other2, pre2, act2, slope_out, near_out,
        part_back, other_back, slope2, slope1, load_sems, swap_send, swap_got, share_send, share_got,
        sends, gots, leave_sems, sq_send, sq_got, sq_sems,
    ) = refs[11:]

    in_width, own_hid = w_first.shape
    own_width, hid = w_last_t.shape
    rows = belief.shape[0]
    blocks = part2.shape[0]
    block = hid // blocks

    landing = (belief_t, target_t, w_first, w_middle, w_last_t)
    arrivals = [
        pltpu.make_async_copy(src, dst, load_sems.at[i])
        for i, (src, dst) in enumerate(zip(loads, landing))
    ]
    arrivals[0].start()

    dp, mp = lax.axis_index("dp"), lax.axis_index("mp")
    me = dp * n_mp + mp
    total = n_dp * n_mp

    def side(bit):
        return (dp // (1 << bit)) % 2

    def peer(bit):
        return (dp + (1 - 2 * side(bit)) * (1 << bit), mp)

    sibling = (dp, 1 - mp)
    x, y = (side(bit) for bit in SHARED[FIRST])
    x_peer, y_peer = (peer(bit) for bit in SHARED[FIRST])
    diagonal = (x_peer[0] + y_peer[0] - dp, mp)
    pair_side = {which: side(SHARED[which][0]) for which in (MIDDLE, LAST)}
    pair_peer = {which: peer(SHARED[which][0]) for which in (MIDDLE, LAST)}
    bits = n_dp.bit_length() - 1
    partners = [sibling, diagonal] + [peer(bit) for bit in range(bits)]
    barrier = pltpu.get_barrier_semaphore()
    for partner in partners:
        pl.semaphore_signal(barrier, inc=1, device_id=partner, device_id_type=MESH)
    for i in (2, 3, 4, 1):
        arrivals[i].start()

    def remote(src, dst, sems, k, goal):
        return pltpu.make_async_remote_copy(
            src, dst, sems[0].at[k], sems[1].at[k], device_id=goal, device_id_type=MESH
        )

    share = functools.partial(remote, sems=(share_send, share_got))
    own_shares = 9
    my_rows = pl.ds(pl.multiple_of(mp * (rows // 2), rows // 2), rows // 2)
    relay_goal = (jnp.where(mp == 0, y_peer[0], x_peer[0]), mp)
    bands = [pl.ds(piece[1], piece[2]) for piece in pieces if piece[0] == FIRST]
    nears = []
    for i, goal in enumerate((x_peer, y_peer)):
        nears.append([
            share(
                belief.at[my_rows, band], near_belief.at[i, my_rows, band],
                k=own_shares + 6 * c + i, goal=goal,
            )
            for c, band in enumerate(bands)
        ])
    relays = [
        share(
            near_belief.at[mp, my_rows, band], near_belief.at[2, my_rows, band],
            k=own_shares + 6 * c + 2, goal=relay_goal,
        )
        for c, band in enumerate(bands)
    ]
    passes = [
        [
            share(
                near_belief.at[i, my_rows, band], near_belief.at[i, my_rows, band],
                k=own_shares + 6 * c + 3 + i, goal=sibling,
            )
            for i in range(3)
        ]
        for c, band in enumerate(bands)
    ]
    slopes = [
        share(parts_t[FIRST].at[at], near_t[FIRST].at[i], k=i, goal=goal)
        for i, (at, goal) in enumerate(
            (((1 - x, y), x_peer), ((x, 1 - y), y_peer), ((1 - x, 1 - y), diagonal))
        )
    ]
    send_act1 = share(act1, near_act1, k=3, goal=pair_peer[MIDDLE])
    send_act2 = share(
        parts_t[LAST].at[1 - pair_side[LAST], mp], near_t[LAST].at[mp], k=4, goal=pair_peer[LAST]
    )
    send_out = share(slope_out, near_out, k=5, goal=pair_peer[LAST])
    send_slope2 = share(
        parts_t[MIDDLE].at[1 - pair_side[MIDDLE], mp], near_t[MIDDLE].at[mp], k=6,
        goal=pair_peer[MIDDLE],
    )
    pass_act2 = share(near_t[LAST].at[mp], near_t[LAST].at[mp], k=7, goal=sibling)
    pass_slope2 = share(near_t[MIDDLE].at[mp], near_t[MIDDLE].at[mp], k=8, goal=sibling)

    def swap(way, part, other, i):
        return pltpu.make_async_remote_copy(
            part.at[i], other.at[i], swap_send.at[way, i], swap_got.at[way, i],
            device_id=sibling, device_id_type=MESH,
        )

    def transpose_parts(which, source, width):
        order = SHARED[which] + tuple(b for b in range(bits) if b not in SHARED[which])
        r = width // n_dp
        step = math.lcm(r, LANES)
        for start in range(0, width, step):
            value = source[:, start : start + step].T
            for d in range(start // r, (start + step) // r):
                where = [(d >> bit) & 1 for bit in order]
                at = 0
                for bit in where[2:]:
                    at = 2 * at + bit
                parts_t[which][where[0], where[1], at * r : (at + 1) * r, :] = value[
                    d * r - start : (d + 1) * r - start
                ]

    def leave(p):
        which, start, width = pieces[p][:3]
        return pltpu.make_async_copy(
            finals[p], outs[which].at[:, pl.ds(start, width)], leave_sems.at[p]
        )

    def dot(left, right):
        return jnp.dot(left, right, preferred_element_type=jnp.float32)

    def first_grad(p):
        start, width = pieces[p][1:3]
        cols = slice(start, start + width)
        value = dot(parts_t[FIRST][x, y], belief[:, cols])
        for i in range(3):
            value = value + dot(near_t[FIRST][i], near_belief[i, :, cols])
        h = value.shape[0] // 2
        store(p, 0, 0, value[:h])
        store(p, 0, 1, value[h:])
        exchange(p, 0).start()

    rights = {MIDDLE: (act1, near_act1), LAST: (slope_out, near_out)}

    def half_grad(p, half):
        which, start, width, order, _, _ = pieces[p]
        own, near = rights[which]
        cols = slice(start, start + width)
        value = dot(parts_t[which][pair_side[which], half], own[:, cols])
        value = value + dot(near_t[which][half], near[:, cols])
        if order[0] == 0:
            store(p, 0, half, value)
        else:
            h = value.shape[0] // 2
            held[p][0][0, half] = value[:h].astype(jnp.bfloat16)
            held[p][0][1, half] = value[h:].astype(jnp.bfloat16)

    def grad(p):
        if pieces[p][0] == FIRST:
            first_grad(p)
        elif pieces[p][3][0] == 0:
            half_grad(p, 1 - x)
            exchange(p, 0).start()
            half_grad(p, x)
        else:
            half_grad(p, 0)
            half_grad(p, 1)
            exchange(p, 0).start()

    def stages_of(p):
        return len(pieces[p][3])

    def store(p, k, half, value):
        ref = held[p][k]
        if k == stages_of(p) - 1:
            ref[half] = value.astype(jnp.bfloat16)
            return
        h = value.shape[0] // 2
        ref[half, 0] = value[:h].astype(jnp.bfloat16)
        ref[half, 1] = value[h:].astype(jnp.bfloat16)

    def exchange(p, k):
        bit = pieces[p][3][k]
        return pltpu.make_async_remote_copy(
            held[p][k].at[1 - side(bit)], got[p][k], sends.at[p, k], gots.at[p, k],
            device_id=peer(bit), device_id_type=MESH,
        )

    def turn(got_first, then):
        for copy in got_first:
            copy.wait_recv()
        for copy in then:
            copy.start()

    def hand_on(c):
        turn((nears[0][c], nears[1][c]), (relays[c], passes[c][0], passes[c][1]))

    arrivals[0].wait()
    for start in range(0, belief.shape[1], LANES * 3):
        value = belief_t[start : min(start + LANES * 3, in_width), :]
        if value.shape[0] < LANES * 3:
            value = jnp.concatenate(
                [value, jnp.zeros((LANES * 3 - value.shape[0], rows), jnp.bfloat16)], axis=0
            )
        belief[:, start : start + LANES * 3] = value.T
    pl.semaphore_wait(barrier, len(partners))
    early = len(bands) - 1
    for c in range(early):
        nears[0][c].start()
        nears[1][c].start()
    arrivals[2].wait()
    for c in range(0, own_hid, 256):
        value = jnp.dot(
            belief[:, :in_width], w_first[:, c : c + 256], preferred_element_type=jnp.float32
        )
        pre1[:, c : c + 256] = value
        act1[:, c : c + 256] = jax.nn.silu(value).astype(jnp.bfloat16)
    send_act1.start()
    arrivals[3].wait()
    for i in range(blocks):
        part2[i] = jnp.dot(
            act1[...], w_middle[:, i * block : (i + 1) * block],
            preferred_element_type=jnp.float32,
        )
        swap(0, part2, other2, i).start()
    arrivals[1].wait()
    arrivals[4].wait()
    row = lax.broadcasted_iota(jnp.int32, (rows, 1), 0)
    limit = jnp.full((rows, 1), counts[0], jnp.int32)
    for b in range(1, rows // BLOCK):
        limit = jnp.where(row >= b * BLOCK, counts[b] + b * BLOCK, limit)
    live = jnp.where(row < limit, 1.0, 0.0)
    target = target_t[...].T
    wanted = target[:, :own_width].astype(jnp.float32)
    for m in range(1, n_mp):
        wanted = jnp.where(
            mp == m, target[:, m * own_width : (m + 1) * own_width].astype(jnp.float32), wanted
        )
    for i in range(blocks):
        cols = slice(i * block, (i + 1) * block)
        swap(0, part2, other2, i).wait_recv()
        value = part2[i] + other2[i]
        pre2[:, cols] = value
        act2[:, cols] = jax.nn.silu(value).astype(jnp.bfloat16)
    transpose_parts(LAST, act2, hid)
    send_act2.start()
    predicted = lax.dot_general(act2[...], w_last_t[...], NT, preferred_element_type=jnp.float32)
    value = jnp.clip(predicted - wanted, -1.0, 1.0) * live
    slope_out[...] = jnp.concatenate(
        [value, jnp.zeros((rows, slope_out.shape[1] - own_width), jnp.float32)], axis=1
    ).astype(jnp.bfloat16)
    hand_on(0)

    for i in range(blocks):
        part_back[i] = jnp.dot(
            slope_out[:, :own_width], w_last_t[:, i * block : (i + 1) * block],
            preferred_element_type=jnp.float32,
        )
        swap(1, part_back, other_back, i).start()
    for i in range(blocks):
        cols = slice(i * block, (i + 1) * block)
        swap(1, part_back, other_back, i).wait_recv()
        value = (part_back[i] + other_back[i]) * silu_slope(pre2[:, cols])
        slope2[:, cols] = value.astype(jnp.bfloat16)
    transpose_parts(MIDDLE, slope2, hid)
    send_slope2.start()
    for c in range(0, own_hid, 256):
        back = lax.dot_general(
            slope2[...], w_middle[c : c + 256, :], NT, preferred_element_type=jnp.float32
        )
        slope1[:, c : c + 256] = (back * silu_slope(pre1[:, c : c + 256])).astype(jnp.bfloat16)
    transpose_parts(FIRST, slope1, own_hid)
    for copy in slopes:
        copy.start()
    for c in range(early, len(bands)):
        nears[0][c].start()
        nears[1][c].start()

    def step(p, k):
        mine = side(pieces[p][3][k])
        exchange(p, k).wait_recv()
        for h in range(2):
            value = held[p][k][mine, h].astype(jnp.float32) + got[p][k][h].astype(jnp.float32)
            store(p, k + 1, h, value)
        exchange(p, k + 1).start()

    def finish(p, k):
        mine = side(pieces[p][3][k])
        exchange(p, k).wait_recv()
        value = held[p][k][mine].astype(jnp.float32) + got[p][k][...].astype(jnp.float32)
        finals[p][...] = value
        leave(p).start()
        across = jnp.sum(value * value, axis=0, keepdims=True)
        for start in range(0, value.shape[1], LANES):
            squares.append(across[:, start : start + LANES])

    squares = []
    actions = [
        (15, turn, ([relays[0]], [passes[0][2]])),
        (18.7, turn, (slopes + passes[0], [])),
        (11.9, turn, ([], [send_out])),
        (21.8, turn, ([send_act2], [pass_act2])),
        (25.3, turn, ([send_slope2], [pass_slope2])),
        (26.9, turn, ([send_act1, pass_slope2], [])),
        (34.3, turn, ([pass_act2, send_out], [])),
    ]
    for c in range(1, len(bands)):
        seen = 12.1 + 0.6 * c if c < early else 22.4
        actions.append((seen, hand_on, (c,)))
        actions.append((22.2 + 1.9 * c, turn, ([relays[c]], [passes[c][2]])))
        actions.append((23.9 + 1.9 * c, turn, (passes[c], [])))
    for p in range(count):
        actions.append((pieces[p][4], grad, (p,)))
        for k in range(stages_of(p)):
            does = step if k < stages_of(p) - 1 else finish
            actions.append((pieces[p][5][k], does, (p, k)))
    for _, does, what in sorted(actions, key=lambda action: action[0]):
        does(*what)
    squares = jnp.sum(sum(squares[1:], squares[0]), axis=1, keepdims=True)

    sq_send[...] = jnp.broadcast_to(squares, sq_send.shape)

    k = 0
    for shift in range(n_dp - 1, -1, -1):
        chip = dp + shift
        chip = jnp.where(chip >= n_dp, chip - n_dp, chip)
        for core in (mp, 1 - mp) if shift else (1 - mp,):
            pltpu.make_async_remote_copy(
                sq_send, sq_got.at[k], sq_sems.at[0], sq_sems.at[1],
                device_id=(chip, core), device_id_type=MESH,
            ).start()
            k += 1
    for i in range(blocks):
        swap(0, part2, other2, i).wait_send()
        swap(1, part_back, other_back, i).wait_send()
    for copy in (
        *nears[0], *nears[1], *relays, *sum(passes, []), *slopes,
        send_act1, send_act2, send_out, send_slope2, pass_act2, pass_slope2,
    ):
        copy.wait_send()
    for p in range(count):
        for k in range(stages_of(p)):
            exchange(p, k).wait_send()
        leave(p).wait()
    pltpu.make_async_copy(sq_got, sq_got, sq_sems.at[1]).wait()
    everyone = squares + jnp.sum(sq_got[...], axis=0)
    scale_out[...] = jnp.broadcast_to(lax.rsqrt(everyone / params + 1e-06), scale_out.shape)
    pltpu.make_async_copy(sq_got, sq_got, sq_sems.at[0]).wait()


def scale_kernel(scale, *refs):
    factor = scale[0:1, 0:1]
    for raw, out in zip(refs[:3], refs[3:]):
        out[...] = raw[:, : out.shape[1]] * factor


def per_device(dims, belief, target_value, counts, w_first, w_middle, w_last):
    n_dp, n_mp = dims
    blocks = 3
    rows, (in_width, own_hid) = belief.shape[0], w_first.shape
    hid, own_width = w_last.shape
    params = float(n_mp * (w_first.size + w_middle.size + w_last.size))
    long = {FIRST: own_hid, MIDDLE: hid, LAST: hid}
    wide = {
        FIRST: pad_to(in_width, LANES),
        MIDDLE: pad_to(own_hid, LANES),
        LAST: pad_to(own_width, LANES),
    }
    layers = (FIRST, MIDDLE, LAST)
    pieces = pieces_of(n_dp, wide)
    half, single = jnp.bfloat16, jnp.float32

    def stage_shapes(piece):
        stages = len(piece[3])
        for k in range(stages):
            r = long[piece[0]] >> (len(SHARED[piece[0]]) + k + 1)
            yield (2, r, piece[2]) if k == stages - 1 else (2, 2, r // 2, piece[2])

    shapes = [list(stage_shapes(piece)) for piece in pieces]
    shares = 9 + 6 * sum(piece[0] == FIRST for piece in pieces)
    deepest = max(len(stages) for stages in shapes)
    loads = (belief.T, target_value.T, w_first, w_middle, w_last.T)
    swapped = pltpu.VMEM((blocks, rows, hid // blocks), single)
    count = len(pieces)
    raws = pl.pallas_call(
        functools.partial(step_kernel, dims, params, pieces, shapes),
        out_shape=[
            jax.ShapeDtypeStruct((long[w] // n_dp, wide[w]), single) for w in layers
        ] + [jax.ShapeDtypeStruct((8, LANES), single)],
        in_specs=[pl.BlockSpec(memory_space=pltpu.SMEM)]
        + [pl.BlockSpec(memory_space=pl.ANY)] * 5,
        out_specs=[pl.BlockSpec(memory_space=pl.ANY)] * 3
        + [pl.BlockSpec(memory_space=pltpu.VMEM)],
        scratch_shapes=(
            [pltpu.VMEM(s, half) for stages in shapes for s in stages]
            + [pltpu.VMEM(s[1:], half) for stages in shapes for s in stages]
            + [pltpu.VMEM(stages[-1][1:], single) for stages in shapes]
            + [
                pltpu.VMEM((in_width, rows), half),
                pltpu.VMEM((n_mp * own_width, rows), half),
                pltpu.VMEM(w_first.shape, half),
                pltpu.VMEM(w_middle.shape, half),
                pltpu.VMEM((own_width, hid), half),
            ]
            + [pltpu.VMEM((2, 2, long[w] // 4, rows), half) for w in layers]
            + [pltpu.VMEM((3 if w == FIRST else 2, long[w] // 4, rows), half) for w in layers]
            + [
                pltpu.VMEM((rows, wide[FIRST]), half),
                pltpu.VMEM((3, rows, wide[FIRST]), half),
                pltpu.VMEM((rows, own_hid), single),
                pltpu.VMEM((rows, own_hid), half),
                pltpu.VMEM((rows, own_hid), half),
                swapped,
                swapped,
                pltpu.VMEM((rows, hid), single),
                pltpu.VMEM((rows, hid), half),
                pltpu.VMEM((rows, wide[LAST]), half),
                pltpu.VMEM((rows, wide[LAST]), half),
                swapped,
                swapped,
                pltpu.VMEM((rows, hid), half),
                pltpu.VMEM((rows, own_hid), half),
                pltpu.SemaphoreType.DMA((5,)),
                pltpu.SemaphoreType.DMA((2, blocks)),
                pltpu.SemaphoreType.DMA((2, blocks)),
                pltpu.SemaphoreType.DMA((shares,)),
                pltpu.SemaphoreType.DMA((shares,)),
                pltpu.SemaphoreType.DMA((count, deepest)),
                pltpu.SemaphoreType.DMA((count, deepest)),
                pltpu.SemaphoreType.DMA((count,)),
                pltpu.VMEM((1, LANES), single),
                pltpu.VMEM((n_dp * n_mp - 1, 1, LANES), single),
                pltpu.SemaphoreType.DMA((2,)),
            ]
        ),
        compiler_params=pltpu.CompilerParams(
            collective_id=0, has_side_effects=True, vmem_limit_bytes=105 * 512 * 1024
        ),
    )(counts, *loads)
    ends = (
        (long[FIRST] // n_dp, in_width),
        (long[MIDDLE] // n_dp, own_hid),
        (long[LAST] // n_dp, own_width),
    )
    first, middle, last = pl.pallas_call(
        scale_kernel,
        out_shape=[jax.ShapeDtypeStruct(s, single) for s in ends],
        in_specs=[pl.BlockSpec(memory_space=pltpu.VMEM)] * 4,
        out_specs=[pl.BlockSpec(memory_space=pltpu.VMEM)] * 3,
        compiler_params=pltpu.CompilerParams(vmem_limit_bytes=4 * 1024 * 1024),
    )(raws[3], *raws[:3])
    return first.T, middle.T, last


def solution(mesh):
    return jax.shard_map(
        functools.partial(per_device, (mesh.shape["dp"], mesh.shape["mp"])),
        mesh=mesh,
        in_specs=(
            P("dp", None),
            P("dp", None),
            P("dp"),
            P(None, "mp"),
            P("mp", None),
            P(None, "mp"),
        ),
        out_specs=(P(None, ("mp", "dp")), P("mp", "dp"), P("dp", "mp")),
        check_vma=False,
    )
```

```python
import functools
import math

import jax
import jax.numpy as jnp
from jax import lax
from jax.experimental import pallas as pl
from jax.experimental.pallas import tpu as pltpu
from jax.sharding import PartitionSpec as P

BLOCK = 128
LANES = 128
MESH = pl.DeviceIdType.MESH
FIRST, MIDDLE, LAST = 0, 1, 2
NT = (((1,), (1,)), ((), ()))


def silu_slope(pre_act):
    sigmoid_of = jax.nn.sigmoid(pre_act)
    return sigmoid_of * (1.0 + pre_act * (1.0 - sigmoid_of))


def pad_to(size, step):
    return -(-size // step) * step


SHARED = {FIRST: (0, 1), MIDDLE: (2,), LAST: (3,)}
PIECES = (
    (LAST, (0, 1), 1, 34.4, (38.2, 43.4, 53)),
    (LAST, (1, 0), 1, 34.5, (38.3, 43.5, 53.1)),
    (LAST, (0, 1), 2, 34.6, (42.4, 46.2, 54)),
    (LAST, (1, 0), 2, 34.7, (42.5, 46.3, 54.1)),
    (FIRST, (2,), 5, 18.8, (36.2, 50)),
    (FIRST, (2,), 6, 25.9, (38.7, 50.1)),
    (FIRST, (2,), 5, 27.8, (41.4, 51)),
    (FIRST, (2,), 5, 29.6, (44.6, 52)),
    (MIDDLE, (1, 0), 1, 27, (30.8, 36, 49)),
    (MIDDLE, (0, 1), 1, 27.1, (30.9, 36.1, 49.1)),
    (MIDDLE, (1, 0), 2, 27.2, (35, 38.8, 50.5)),
    (MIDDLE, (0, 1), 2, 27.3, (35.1, 38.9, 50.6)),
)


def pieces_of(n_dp, wide):
    total = n_dp.bit_length() - 1
    out = []
    for which in (LAST, FIRST, MIDDLE):
        mine = [piece for piece in PIECES if piece[0] == which]
        tiles, parts = wide[which] // LANES, [piece[2] for piece in mine]
        bounds = [
            round(tiles * sum(parts[:i]) / sum(parts)) * LANES for i in range(len(mine) + 1)
        ]
        for i, (_, head, _, when, keys) in enumerate(mine):
            tail = [b for b in range(total) if b not in SHARED[which] + head]
            bits = head + tuple(tail)
            more = len(bits) - len(keys)
            keys = keys[:-1] + tuple(keys[-2] + 7 * (j + 1) for j in range(more)) + (keys[-1] + 7 * more,)
            out.append((which, bounds[i], bounds[i + 1] - bounds[i], bits, when, keys))
    return out


def step_kernel(dims, params, pieces, stage_shapes, *refs):
    n_dp, n_mp = dims
    count = len(pieces)
    counts, loads, outs, scale_out = refs[0], refs[1:6], refs[6:9], refs[9]
    refs = refs[10:]
    held, got = [], []
    for group in (held, got):
        for shapes in stage_shapes:
            group.append(refs[: len(shapes)])
            refs = refs[len(shapes) :]
    finals, refs = refs[:count], refs[count:]
    belief_t, target_t, w_first, w_middle, w_last_t = refs[:5]
    parts_t, near_t = refs[5:8], refs[8:11]
    (
        belief, near_belief, pre1, act1, near_act1, part2, other2, pre2, act2, slope_out, near_out,
        part_back, other_back, slope2, slope1, load_sems, swap_send, swap_got, share_send, share_got,
        sends, gots, leave_sems, sq_send, sq_got, sq_sems,
    ) = refs[11:]

    in_width, own_hid = w_first.shape
    own_width, hid = w_last_t.shape
    rows = belief.shape[0]
    blocks = part2.shape[0]
    block = hid // blocks

    landing = (belief_t, target_t, w_first, w_middle, w_last_t)
    arrivals = [
        pltpu.make_async_copy(src, dst, load_sems.at[i])
        for i, (src, dst) in enumerate(zip(loads, landing))
    ]
    arrivals[0].start()

    dp, mp = lax.axis_index("dp"), lax.axis_index("mp")
    me = dp * n_mp + mp
    total = n_dp * n_mp

    def side(bit):
        return (dp // (1 << bit)) % 2

    def peer(bit):
        return (dp + (1 - 2 * side(bit)) * (1 << bit), mp)

    sibling = (dp, 1 - mp)
    x, y = (side(bit) for bit in SHARED[FIRST])
    x_peer, y_peer = (peer(bit) for bit in SHARED[FIRST])
    diagonal = (x_peer[0] + y_peer[0] - dp, mp)
    pair_side = {which: side(SHARED[which][0]) for which in (MIDDLE, LAST)}
    pair_peer = {which: peer(SHARED[which][0]) for which in (MIDDLE, LAST)}
    bits = n_dp.bit_length() - 1
    partners = [sibling, diagonal] + [peer(bit) for bit in range(bits)]
    barrier = pltpu.get_barrier_semaphore()
    for partner in partners:
        pl.semaphore_signal(barrier, inc=1, device_id=partner, device_id_type=MESH)
    for i in (2, 3, 4, 1):
        arrivals[i].start()

    def remote(src, dst, sems, k, goal):
        return pltpu.make_async_remote_copy(
            src, dst, sems[0].at[k], sems[1].at[k], device_id=goal, device_id_type=MESH
        )

    share = functools.partial(remote, sems=(share_send, share_got))
    own_shares = 9
    my_rows = pl.ds(pl.multiple_of(mp * (rows // 2), rows // 2), rows // 2)
    relay_goal = (jnp.where(mp == 0, y_peer[0], x_peer[0]), mp)
    bands = [pl.ds(piece[1], piece[2]) for piece in pieces if piece[0] == FIRST]
    nears = []
    for i, goal in enumerate((x_peer, y_peer)):
        nears.append([
            share(
                belief.at[my_rows, band], near_belief.at[i, my_rows, band],
                k=own_shares + 6 * c + i, goal=goal,
            )
            for c, band in enumerate(bands)
        ])
    relays = [
        share(
            near_belief.at[mp, my_rows, band], near_belief.at[2, my_rows, band],
            k=own_shares + 6 * c + 2, goal=relay_goal,
        )
        for c, band in enumerate(bands)
    ]
    passes = [
        [
            share(
                near_belief.at[i, my_rows, band], near_belief.at[i, my_rows, band],
                k=own_shares + 6 * c + 3 + i, goal=sibling,
            )
            for i in range(3)
        ]
        for c, band in enumerate(bands)
    ]
    slopes = [
        share(parts_t[FIRST].at[at], near_t[FIRST].at[i], k=i, goal=goal)
        for i, (at, goal) in enumerate(
            (((1 - x, y), x_peer), ((x, 1 - y), y_peer), ((1 - x, 1 - y), diagonal))
        )
    ]
    send_act1 = share(act1, near_act1, k=3, goal=pair_peer[MIDDLE])
    send_act2 = share(
        parts_t[LAST].at[1 - pair_side[LAST], mp], near_t[LAST].at[mp], k=4, goal=pair_peer[LAST]
    )
    send_out = share(slope_out, near_out, k=5, goal=pair_peer[LAST])
    send_slope2 = share(
        parts_t[MIDDLE].at[1 - pair_side[MIDDLE], mp], near_t[MIDDLE].at[mp], k=6,
        goal=pair_peer[MIDDLE],
    )
    pass_act2 = share(near_t[LAST].at[mp], near_t[LAST].at[mp], k=7, goal=sibling)
    pass_slope2 = share(near_t[MIDDLE].at[mp], near_t[MIDDLE].at[mp], k=8, goal=sibling)

    def swap(way, part, other, i):
        return pltpu.make_async_remote_copy(
            part.at[i], other.at[i], swap_send.at[way, i], swap_got.at[way, i],
            device_id=sibling, device_id_type=MESH,
        )

    def transpose_parts(which, source, width):
        order = SHARED[which] + tuple(b for b in range(bits) if b not in SHARED[which])
        r = width // n_dp
        step = math.lcm(r, LANES)
        for start in range(0, width, step):
            value = source[:, start : start + step].T
            for d in range(start // r, (start + step) // r):
                where = [(d >> bit) & 1 for bit in order]
                at = 0
                for bit in where[2:]:
                    at = 2 * at + bit
                parts_t[which][where[0], where[1], at * r : (at + 1) * r, :] = value[
                    d * r - start : (d + 1) * r - start
                ]

    def leave(p):
        which, start, width = pieces[p][:3]
        return pltpu.make_async_copy(
            finals[p], outs[which].at[:, pl.ds(start, width)], leave_sems.at[p]
        )

    def dot(left, right):
        return jnp.dot(left, right, preferred_element_type=jnp.float32)

    def first_grad(p):
        start, width = pieces[p][1:3]
        cols = slice(start, start + width)
        value = dot(parts_t[FIRST][x, y], belief[:, cols])
        for i in range(3):
            value = value + dot(near_t[FIRST][i], near_belief[i, :, cols])
        h = value.shape[0] // 2
        store(p, 0, 0, value[:h])
        store(p, 0, 1, value[h:])
        exchange(p, 0).start()

    rights = {MIDDLE: (act1, near_act1), LAST: (slope_out, near_out)}

    def half_grad(p, half):
        which, start, width, order, _, _ = pieces[p]
        own, near = rights[which]
        cols = slice(start, start + width)
        value = dot(parts_t[which][pair_side[which], half], own[:, cols])
        value = value + dot(near_t[which][half], near[:, cols])
        if order[0] == 0:
            store(p, 0, half, value)
        else:
            h = value.shape[0] // 2
            held[p][0][0, half] = value[:h].astype(jnp.bfloat16)
            held[p][0][1, half] = value[h:].astype(jnp.bfloat16)

    def grad(p):
        if pieces[p][0] == FIRST:
            first_grad(p)
        elif pieces[p][3][0] == 0:
            half_grad(p, 1 - x)
            exchange(p, 0).start()
            half_grad(p, x)
        else:
            half_grad(p, 0)
            half_grad(p, 1)
            exchange(p, 0).start()

    def stages_of(p):
        return len(pieces[p][3])

    def store(p, k, half, value):
        ref = held[p][k]
        if k == stages_of(p) - 1:
            ref[half] = value.astype(jnp.bfloat16)
            return
        h = value.shape[0] // 2
        ref[half, 0] = value[:h].astype(jnp.bfloat16)
        ref[half, 1] = value[h:].astype(jnp.bfloat16)

    def exchange(p, k):
        bit = pieces[p][3][k]
        return pltpu.make_async_remote_copy(
            held[p][k].at[1 - side(bit)], got[p][k], sends.at[p, k], gots.at[p, k],
            device_id=peer(bit), device_id_type=MESH,
        )

    def turn(got_first, then):
        for copy in got_first:
            copy.wait_recv()
        for copy in then:
            copy.start()

    def hand_on(c):
        turn((nears[0][c], nears[1][c]), (relays[c], passes[c][0], passes[c][1]))

    arrivals[0].wait()
    early = len(bands) - 1
    ends = [piece[1] + piece[2] for piece in pieces if piece[0] == FIRST]
    gone = 0
    for start in range(0, belief.shape[1], LANES * 3):
        value = belief_t[start : min(start + LANES * 3, in_width), :]
        if value.shape[0] < LANES * 3:
            value = jnp.concatenate(
                [value, jnp.zeros((LANES * 3 - value.shape[0], rows), jnp.bfloat16)], axis=0
            )
        belief[:, start : start + LANES * 3] = value.T
        while gone < early and ends[gone] <= start + LANES * 3:
            if gone == 0:
                pl.semaphore_wait(barrier, len(partners))
            nears[0][gone].start()
            nears[1][gone].start()
            gone += 1
    arrivals[2].wait()
    for c in range(0, own_hid, 256):
        value = jnp.dot(
            belief[:, :in_width], w_first[:, c : c + 256], preferred_element_type=jnp.float32
        )
        pre1[:, c : c + 256] = value
        act1[:, c : c + 256] = jax.nn.silu(value).astype(jnp.bfloat16)
    send_act1.start()
    arrivals[3].wait()
    for i in range(blocks):
        part2[i] = jnp.dot(
            act1[...], w_middle[:, i * block : (i + 1) * block],
            preferred_element_type=jnp.float32,
        )
        swap(0, part2, other2, i).start()
    arrivals[1].wait()
    arrivals[4].wait()
    row = lax.broadcasted_iota(jnp.int32, (rows, 1), 0)
    limit = jnp.full((rows, 1), counts[0], jnp.int32)
    for b in range(1, rows // BLOCK):
        limit = jnp.where(row >= b * BLOCK, counts[b] + b * BLOCK, limit)
    live = jnp.where(row < limit, 1.0, 0.0)
    target = target_t[...].T
    wanted = target[:, :own_width].astype(jnp.float32)
    for m in range(1, n_mp):
        wanted = jnp.where(
            mp == m, target[:, m * own_width : (m + 1) * own_width].astype(jnp.float32), wanted
        )
    for i in range(blocks):
        cols = slice(i * block, (i + 1) * block)
        swap(0, part2, other2, i).wait_recv()
        value = part2[i] + other2[i]
        pre2[:, cols] = value
        act2[:, cols] = jax.nn.silu(value).astype(jnp.bfloat16)
    transpose_parts(LAST, act2, hid)
    send_act2.start()
    predicted = lax.dot_general(act2[...], w_last_t[...], NT, preferred_element_type=jnp.float32)
    value = jnp.clip(predicted - wanted, -1.0, 1.0) * live
    slope_out[...] = jnp.concatenate(
        [value, jnp.zeros((rows, slope_out.shape[1] - own_width), jnp.float32)], axis=1
    ).astype(jnp.bfloat16)
    hand_on(0)

    for i in range(blocks):
        part_back[i] = jnp.dot(
            slope_out[:, :own_width], w_last_t[:, i * block : (i + 1) * block],
            preferred_element_type=jnp.float32,
        )
        swap(1, part_back, other_back, i).start()
    for i in range(blocks):
        cols = slice(i * block, (i + 1) * block)
        swap(1, part_back, other_back, i).wait_recv()
        value = (part_back[i] + other_back[i]) * silu_slope(pre2[:, cols])
        slope2[:, cols] = value.astype(jnp.bfloat16)
    transpose_parts(MIDDLE, slope2, hid)
    send_slope2.start()
    for c in range(0, own_hid, 256):
        back = lax.dot_general(
            slope2[...], w_middle[c : c + 256, :], NT, preferred_element_type=jnp.float32
        )
        slope1[:, c : c + 256] = (back * silu_slope(pre1[:, c : c + 256])).astype(jnp.bfloat16)
    transpose_parts(FIRST, slope1, own_hid)
    for copy in slopes:
        copy.start()
    for c in range(early, len(bands)):
        nears[0][c].start()
        nears[1][c].start()

    def step(p, k):
        mine = side(pieces[p][3][k])
        exchange(p, k).wait_recv()
        for h in range(2):
            value = held[p][k][mine, h].astype(jnp.float32) + got[p][k][h].astype(jnp.float32)
            store(p, k + 1, h, value)
        exchange(p, k + 1).start()

    def finish(p, k):
        mine = side(pieces[p][3][k])
        exchange(p, k).wait_recv()
        value = held[p][k][mine].astype(jnp.float32) + got[p][k][...].astype(jnp.float32)
        finals[p][...] = value
        leave(p).start()
        across = jnp.sum(value * value, axis=0, keepdims=True)
        for start in range(0, value.shape[1], LANES):
            squares.append(across[:, start : start + LANES])

    squares = []
    actions = [
        (15, turn, ([relays[0]], [passes[0][2]])),
        (18.7, turn, (slopes + passes[0], [])),
        (11.9, turn, ([], [send_out])),
        (21.8, turn, ([send_act2], [pass_act2])),
        (25.3, turn, ([send_slope2], [pass_slope2])),
        (26.9, turn, ([send_act1, pass_slope2], [])),
        (34.3, turn, ([pass_act2, send_out], [])),
    ]
    for c in range(1, len(bands)):
        seen = 12.1 + 0.6 * c if c < early else 22.4
        actions.append((seen, hand_on, (c,)))
        actions.append((22.2 + 1.9 * c, turn, ([relays[c]], [passes[c][2]])))
        actions.append((23.9 + 1.9 * c, turn, (passes[c], [])))
    for p in range(count):
        actions.append((pieces[p][4], grad, (p,)))
        for k in range(stages_of(p)):
            does = step if k < stages_of(p) - 1 else finish
            actions.append((pieces[p][5][k], does, (p, k)))
    for _, does, what in sorted(actions, key=lambda action: action[0]):
        does(*what)
    squares = jnp.sum(sum(squares[1:], squares[0]), axis=1, keepdims=True)

    sq_send[...] = jnp.broadcast_to(squares, sq_send.shape)

    k = 0
    for shift in range(n_dp - 1, -1, -1):
        chip = dp + shift
        chip = jnp.where(chip >= n_dp, chip - n_dp, chip)
        for core in (mp, 1 - mp) if shift else (1 - mp,):
            pltpu.make_async_remote_copy(
                sq_send, sq_got.at[k], sq_sems.at[0], sq_sems.at[1],
                device_id=(chip, core), device_id_type=MESH,
            ).start()
            k += 1
    for i in range(blocks):
        swap(0, part2, other2, i).wait_send()
        swap(1, part_back, other_back, i).wait_send()
    for copy in (
        *nears[0], *nears[1], *relays, *sum(passes, []), *slopes,
        send_act1, send_act2, send_out, send_slope2, pass_act2, pass_slope2,
    ):
        copy.wait_send()
    for p in range(count):
        for k in range(stages_of(p)):
            exchange(p, k).wait_send()
        leave(p).wait()
    pltpu.make_async_copy(sq_got, sq_got, sq_sems.at[1]).wait()
    everyone = squares + jnp.sum(sq_got[...], axis=0)
    scale_out[...] = jnp.broadcast_to(lax.rsqrt(everyone / params + 1e-06), scale_out.shape)
    pltpu.make_async_copy(sq_got, sq_got, sq_sems.at[0]).wait()


def scale_kernel(scale, *refs):
    factor = scale[0:1, 0:1]
    for raw, out in zip(refs[:3], refs[3:]):
        out[...] = raw[:, : out.shape[1]] * factor


def per_device(dims, belief, target_value, counts, w_first, w_middle, w_last):
    n_dp, n_mp = dims
    blocks = 3
    rows, (in_width, own_hid) = belief.shape[0], w_first.shape
    hid, own_width = w_last.shape
    params = float(n_mp * (w_first.size + w_middle.size + w_last.size))
    long = {FIRST: own_hid, MIDDLE: hid, LAST: hid}
    wide = {
        FIRST: pad_to(in_width, LANES),
        MIDDLE: pad_to(own_hid, LANES),
        LAST: pad_to(own_width, LANES),
    }
    layers = (FIRST, MIDDLE, LAST)
    pieces = pieces_of(n_dp, wide)
    half, single = jnp.bfloat16, jnp.float32

    def stage_shapes(piece):
        stages = len(piece[3])
        for k in range(stages):
            r = long[piece[0]] >> (len(SHARED[piece[0]]) + k + 1)
            yield (2, r, piece[2]) if k == stages - 1 else (2, 2, r // 2, piece[2])

    shapes = [list(stage_shapes(piece)) for piece in pieces]
    shares = 9 + 6 * sum(piece[0] == FIRST for piece in pieces)
    deepest = max(len(stages) for stages in shapes)
    loads = (belief.T, target_value.T, w_first, w_middle, w_last.T)
    swapped = pltpu.VMEM((blocks, rows, hid // blocks), single)
    count = len(pieces)
    raws = pl.pallas_call(
        functools.partial(step_kernel, dims, params, pieces, shapes),
        out_shape=[
            jax.ShapeDtypeStruct((long[w] // n_dp, wide[w]), single) for w in layers
        ] + [jax.ShapeDtypeStruct((8, LANES), single)],
        in_specs=[pl.BlockSpec(memory_space=pltpu.SMEM)]
        + [pl.BlockSpec(memory_space=pl.ANY)] * 5,
        out_specs=[pl.BlockSpec(memory_space=pl.ANY)] * 3
        + [pl.BlockSpec(memory_space=pltpu.VMEM)],
        scratch_shapes=(
            [pltpu.VMEM(s, half) for stages in shapes for s in stages]
            + [pltpu.VMEM(s[1:], half) for stages in shapes for s in stages]
            + [pltpu.VMEM(stages[-1][1:], single) for stages in shapes]
            + [
                pltpu.VMEM((in_width, rows), half),
                pltpu.VMEM((n_mp * own_width, rows), half),
                pltpu.VMEM(w_first.shape, half),
                pltpu.VMEM(w_middle.shape, half),
                pltpu.VMEM((own_width, hid), half),
            ]
            + [pltpu.VMEM((2, 2, long[w] // 4, rows), half) for w in layers]
            + [pltpu.VMEM((3 if w == FIRST else 2, long[w] // 4, rows), half) for w in layers]
            + [
                pltpu.VMEM((rows, wide[FIRST]), half),
                pltpu.VMEM((3, rows, wide[FIRST]), half),
                pltpu.VMEM((rows, own_hid), single),
                pltpu.VMEM((rows, own_hid), half),
                pltpu.VMEM((rows, own_hid), half),
                swapped,
                swapped,
                pltpu.VMEM((rows, hid), single),
                pltpu.VMEM((rows, hid), half),
                pltpu.VMEM((rows, wide[LAST]), half),
                pltpu.VMEM((rows, wide[LAST]), half),
                swapped,
                swapped,
                pltpu.VMEM((rows, hid), half),
                pltpu.VMEM((rows, own_hid), half),
                pltpu.SemaphoreType.DMA((5,)),
                pltpu.SemaphoreType.DMA((2, blocks)),
                pltpu.SemaphoreType.DMA((2, blocks)),
                pltpu.SemaphoreType.DMA((shares,)),
                pltpu.SemaphoreType.DMA((shares,)),
                pltpu.SemaphoreType.DMA((count, deepest)),
                pltpu.SemaphoreType.DMA((count, deepest)),
                pltpu.SemaphoreType.DMA((count,)),
                pltpu.VMEM((1, LANES), single),
                pltpu.VMEM((n_dp * n_mp - 1, 1, LANES), single),
                pltpu.SemaphoreType.DMA((2,)),
            ]
        ),
        compiler_params=pltpu.CompilerParams(
            collective_id=0, has_side_effects=True, vmem_limit_bytes=105 * 512 * 1024
        ),
    )(counts, *loads)
    ends = (
        (long[FIRST] // n_dp, in_width),
        (long[MIDDLE] // n_dp, own_hid),
        (long[LAST] // n_dp, own_width),
    )
    first, middle, last = pl.pallas_call(
        scale_kernel,
        out_shape=[jax.ShapeDtypeStruct(s, single) for s in ends],
        in_specs=[pl.BlockSpec(memory_space=pltpu.VMEM)] * 4,
        out_specs=[pl.BlockSpec(memory_space=pltpu.VMEM)] * 3,
        compiler_params=pltpu.CompilerParams(vmem_limit_bytes=4 * 1024 * 1024),
    )(raws[3], *raws[:3])
    return first.T, middle.T, last


def solution(mesh):
    return jax.shard_map(
        functools.partial(per_device, (mesh.shape["dp"], mesh.shape["mp"])),
        mesh=mesh,
        in_specs=(
            P("dp", None),
            P("dp", None),
            P("dp"),
            P(None, "mp"),
            P("mp", None),
            P(None, "mp"),
        ),
        out_specs=(P(None, ("mp", "dp")), P("mp", "dp"), P("dp", "mp")),
        check_vma=False,
    )
```
